256 devices in a mesh: dom: 16 (over z, y_lo), edge: 16 (over x, y_hi, core).
Axes of the slice: x: 4, y: 4 (y_hi: 2, y_lo: 2; y = y_hi * 2 + y_lo), z: 8, core: 2. Of those that a mesh axis runs over, the one named last changes fastest.
Arguments:
- src_table: float32 [4096, 400], P(('dom', 'edge')), may hold values from -6 to 6
- src_state: float32 [4096], P(('dom', 'edge')), may hold values from 0.1 to 30
- dst_table: float32 [4096, 400], P(('dom', 'edge')), may hold values from -6 to 6
- dst_state: float32 [4096], P(('dom', 'edge')), may hold values from 0.1 to 30
- relations: float32 [4131, 400], replicated, may hold values from -1.5 to 1.5
- edge_src: int32 [2, 128000], P(None, ('dom', 'edge')), may hold values from 0 to 255
- edge_rel: int32 [2, 128000], P(None, ('dom', 'edge')), may hold values from 0 to 4130
- edge_dst: int32 [2, 128000], P(None, ('dom', 'edge')), may hold values from 0 to 255
- negatives: int32 [2, 256, 500], P(None, ('dom', 'edge')), may hold values from 0 to 255
Outputs:
- src_out: float32 [4096, 400], P(('dom', 'edge'))
- src_state_out: float32 [4096], P(('dom', 'edge'))
- dst_out: float32 [4096, 400], P(('dom', 'edge'))
- dst_state_out: float32 [4096], P(('dom', 'edge'))
The draws below stay inside these ranges and needn't reach their ends.
All inputs are finite; a program needn't handle non-finite values.
Results may differ from the reference program's by a relative error of at most 0.00013.
Values sent between devices are 32-bit elements; how exact they have to be, the bound alone decides.
A program may use at most 64 MiB of HBM per device.

```python
import math
import jax
import jax.numpy as jnp
import numpy as np
from jax import lax

D = 400
NREL = 4131
NEG = 500
ENT = 256
NENT = 4096
EDGES = 128000
NSPANS = 256
N_DOM = 16


def touch_ends(result, stream_key, least, largest):
    dims = result.shape
    spot = [jax.random.randint(jax.random.fold_in(stream_key, axis), (), 0, dims[axis]) for axis in range(len(dims))]
    result = result.at[tuple(spot)].set(least)
    longest = dims.index(max(dims))
    spot[longest] = (spot[longest] + 1) % dims[longest]
    return result.at[tuple(spot)].set(largest)


def block_scale(stream_key, shape, pieces, smallest, top_value):
    factor_of = 1.0
    for position, parts in pieces:
        heights = jax.random.uniform(jax.random.fold_in(jax.random.fold_in(stream_key, 6), position), (parts,), jnp.float32, smallest / len(pieces), top_value / len(pieces))
        factor_of = factor_of * jnp.repeat(jnp.exp(heights), shape[position] // parts).reshape((-1,) + (1,) * (len(shape) - 1 - position))
    return factor_of


def rank_bounds(amount, slope):
    portions = [(1 << 20) // math.isqrt(standing ** slope) + 1 for standing in range(1, amount + 1)]
    spread = 1 + sum(portions) // (1 << 30)
    return np.cumsum(np.array([max(1, weight // spread) for weight in portions]))


def ranked(own_key, dims, amount, skew):
    listing = rank_bounds(amount, skew)
    lot = jax.random.randint(jax.random.fold_in(own_key, 1), dims, 0, int(listing[amount - 1]))
    grade = jnp.searchsorted(jnp.asarray(listing, jnp.int32), lot, side="right")
    return jax.random.permutation(jax.random.fold_in(own_key, 2), amount)[grade].astype(jnp.int32)


def centred(rng, shape, scale, most, pieces=(), dtype=jnp.bfloat16):
    drawn = jax.random.normal(rng, shape, jnp.float32) * scale
    if len(pieces) > 0:
        drawn = block_scale(rng, shape, pieces, -0.22, 0.18) * drawn
    return jnp.clip(drawn, min=-most, max=most).astype(dtype)


def setup_inputs(seed: int = 0) -> dict:
    splits = jax.random.split(jax.random.key(seed), 10)
    return {
        "src_table": centred(splits[0], (NENT, D), 1.0, 6.0, ((0, 256),), jnp.float32),
        "src_state": jnp.clip(jnp.exp(math.log(30.0) - 5.7037825 * jax.random.uniform(splits[1], (NENT,), jnp.float32) ** block_scale(splits[1], (NENT,), ((0, 256),), -0.2, 0.2)), 0.1, 30.0),
        "dst_table": centred(splits[2], (NENT, D), 1.0, 6.0, ((0, 256),), jnp.float32),
        "dst_state": jnp.clip(jnp.exp(math.log(30.0) - 5.7037825 * jax.random.uniform(splits[3], (NENT,), jnp.float32) ** block_scale(splits[3], (NENT,), ((0, 256),), -0.2, 0.2)), 0.1, 30.0),
        "relations": centred(splits[4], (NREL, D), 0.3, 1.5, (), jnp.float32),
        "edge_src": touch_ends(jax.random.randint(splits[5], (2, EDGES), 0, ENT), jax.random.fold_in(splits[5], 1), 0, ENT - 1).astype(jnp.int32),
        "edge_rel": touch_ends(ranked(splits[6], (2, EDGES), NREL, 2), jax.random.fold_in(splits[6], 3), 0, NREL - 1).astype(jnp.int32),
        "edge_dst": touch_ends(jax.random.randint(splits[7], (2, EDGES), 0, ENT), jax.random.fold_in(splits[7], 1), 0, ENT - 1).astype(jnp.int32),
        "negatives": touch_ends(jax.random.randint(splits[8], (2, NSPANS, NEG), 0, ENT), jax.random.fold_in(splits[8], 1), 0, ENT - 1).astype(jnp.int32),
    }


learn_rate = 0.1
epsilon = 1e-06

def bucket_grads(source_rows, target_rows, relations, src_ids, rel_ids, dst_ids, neg_ids):
    middle = source_rows.shape[1] // 2
    blocks = neg_ids.shape[0]
    source = jnp.take(source_rows, src_ids, axis=0)
    target = jnp.take(target_rows, dst_ids, axis=0)
    relation = jnp.take(relations, rel_ids, axis=0)
    src_real, src_imag = (source[:, :middle], source[:, middle:])
    rel_real, rel_imag = (relation[:, :middle], relation[:, middle:])
    rotated = jnp.concatenate([src_real * rel_real - src_imag * rel_imag, src_real * rel_imag + src_imag * rel_real], axis=1)
    positive = lax.optimization_barrier(jnp.sum(rotated * target, axis=1))
    grouped = rotated.reshape(blocks, -1, rotated.shape[1])
    sampled = jnp.take(target_rows, neg_ids, axis=0)
    negative = jnp.einsum('cen,ckn->cek', grouped, sampled, precision=lax.Precision.HIGHEST)
    pos_weight = -jax.nn.sigmoid(-positive)
    neg_weight = jax.nn.sigmoid(negative)
    from_negs = jnp.einsum('cek,ckn->cen', neg_weight, sampled, precision=lax.Precision.HIGHEST)
    rotated_grad = pos_weight[:, None] * target + from_negs.reshape(rotated.shape)
    sampled_grad = jnp.einsum('cek,cen->ckn', neg_weight, grouped, precision=lax.Precision.HIGHEST)
    grad_real, grad_imag = (rotated_grad[:, :middle], rotated_grad[:, middle:])
    source_grad = jnp.concatenate([grad_real * rel_real + grad_imag * rel_imag, grad_imag * rel_real - grad_real * rel_imag], axis=1)
    src_sum = jnp.zeros_like(source_rows).at[src_ids].add(source_grad)
    dst_sum = jnp.zeros_like(target_rows).at[dst_ids].add(pos_weight[:, None] * rotated)
    dst_sum = dst_sum.at[neg_ids.reshape(-1)].add(sampled_grad.reshape(-1, sampled_grad.shape[2]))
    return (src_sum, dst_sum)

def row_adagrad(table, state, grad):
    state = state + lax.optimization_barrier(jnp.mean(grad * grad, axis=-1))
    table = table - learn_rate * grad / (jnp.sqrt(state)[..., None] + epsilon)
    return (table, state)

def reference(src_table, src_state, dst_table, dst_state, relations, edge_src, edge_rel, edge_dst, negatives):
    groups = N_DOM
    width = src_table.shape[1]
    src_parts = src_table.reshape(groups, -1, width)
    src_sums = src_state.reshape(groups, -1)
    dst_parts = dst_table.reshape(groups, -1, width)
    dst_sums = dst_state.reshape(groups, -1)
    edge_sources = edge_src.reshape(2, groups, -1)
    edge_relations = edge_rel.reshape(2, groups, -1)
    edge_targets = edge_dst.reshape(2, groups, -1)
    neg_groups = negatives.reshape(2, groups, -1, negatives.shape[2])
    for bucket in range(2):
        offset = bucket + 1
        dst_turned = jnp.roll(dst_parts, offset, axis=0)
        sums_turned = jnp.roll(dst_sums, offset, axis=0)

        def one_group(items):
            return bucket_grads(items[0], items[1], relations, items[2], items[3], items[4], items[5])
        src_grad, dst_grad = lax.map(one_group, (src_parts, dst_turned, edge_sources[bucket], edge_relations[bucket], edge_targets[bucket], neg_groups[bucket]))
        src_parts, src_sums = row_adagrad(src_parts, src_sums, src_grad)
        dst_turned, sums_turned = row_adagrad(dst_turned, sums_turned, dst_grad)
        dst_parts = jnp.roll(dst_turned, -offset, axis=0)
        dst_sums = jnp.roll(sums_turned, -offset, axis=0)
    return (src_parts.reshape(-1, width), src_sums.reshape(-1), dst_parts.reshape(-1, width), dst_sums.reshape(-1))
```

```python
import functools

import jax
import jax.numpy as jnp
from jax import lax
from jax.experimental import pallas as pl
from jax.experimental.pallas import tpu as pltpu
from jax.sharding import PartitionSpec as P

MESH = pl.DeviceIdType.MESH
LEARN_RATE = 0.1
EPSILON = 1e-06
BF = jnp.bfloat16
F32 = jnp.float32


def up(n, m):
    return (n + m - 1) // m * m


def halves(x):
    hi = x.astype(BF)
    return hi, (x - hi.astype(F32)).astype(BF)


def nn(a, b):
    return jnp.dot(a, b, preferred_element_type=F32)


def nt(a, b):
    return lax.dot_general(a, b, (((1,), (1,)), ((), ())), preferred_element_type=F32)


def kernel(
    doms, chips, half,
    src_ref, sst_ref, dst_ref, dstt_ref, rel_hbm, es_ref, er_ref, ed_ref, ng_ref,
    src_out, sst_out, dst_out, dstt_out,
    rel_v, raw, rsp, hot, hot_t, wgt, pos, ids,
    own_s, own_d, full_s, full_d, part_s, part_d, sib_s, sib_d, sum_s, sum_d, red_s, red_d,
    qh, ql, dh, dl, th, tl, wth, wtl, wh, wl,
    rel_sem, ags_send, ags_recv, agd_send, agd_recv, fws_send, fws_recv, fwd_send, fwd_recv,
    dd_send, dd_recv, rss_send, rss_recv, rsd_send, rsd_recv,
):
    rows = src_ref.shape[0]
    width = src_ref.shape[1]
    hp = up(half, 128)
    wide = 2 * hp
    ents = full_s.shape[1]
    hent = ents // 2
    edges = es_ref.shape[1]
    ep = rsp.shape[1]
    nrel = rel_v.shape[0]
    shift = hp - half

    dom = lax.axis_index("dom")
    k = lax.axis_index("edge")
    core = lax.rem(k, 2)
    chip = lax.div(k, 2)
    mate = chip * 2 + (1 - core)

    def at_dom(step):
        return lax.rem(dom + step + doms, doms)

    def peer(j):
        return lax.rem(chip + j, chips)

    piece = up(-(-nrel // rel_sem.shape[0]), 8)
    rel_copies = []
    for n in range(rel_sem.shape[0]):
        lo = n * piece
        size = min(piece, nrel - lo)
        c = pltpu.make_async_copy(rel_hbm.at[pl.ds(lo, size)], rel_v.at[pl.ds(lo, size)], rel_sem.at[n])
        c.start()
        rel_copies.append(c)

    bar = pltpu.get_barrier_semaphore()
    count = 1
    pl.semaphore_signal(bar, inc=1, device_id=(dom, mate), device_id_type=MESH)
    for j in range(1, chips):
        pl.semaphore_signal(bar, inc=1, device_id=(dom, peer(j) * 2 + core), device_id_type=MESH)
        count += 1
    for other in (at_dom(1), at_dom(-1)):
        for j in range(chips):
            pl.semaphore_signal(bar, inc=1, device_id=(other, peer(j) * 2 + core), device_id_type=MESH)
            count += 1

    lane = lax.broadcasted_iota(jnp.int32, (rows, wide), 1)

    def spread(x_ref, to):
        to[0] = jnp.zeros((rows, wide), F32)
        to[0, :, 0:width] = x_ref[...]
        x = to[0]
        im = pltpu.roll(x, shift, axis=1)
        to[0] = jnp.where(lane < half, x, jnp.where(lane >= hp, im, 0.0))

    def joined(x):
        im = pltpu.roll(x, wide - shift, axis=1)
        return jnp.where(lane < half, x, im)[:, :width]

    spread(src_ref, own_s)
    spread(dst_ref, own_d)

    eye = lax.broadcasted_iota(jnp.int32, (rows, rows), 0) == lax.broadcasted_iota(jnp.int32, (rows, rows), 1)

    def column(x_ref):
        return jnp.sum(jnp.where(eye, jnp.broadcast_to(x_ref[...], (rows, rows)), 0.0), axis=1, keepdims=True)

    def as_row(x):
        return jnp.sum(jnp.where(eye, jnp.broadcast_to(x, (rows, rows)), 0.0), axis=0, keepdims=True)

    src_state = column(sst_ref)
    dst_state = column(dstt_ref)

    my_rows = pl.ds(pl.multiple_of(core * hent + chip * rows, rows), rows)

    def block_of(c):
        return pl.ds(pl.multiple_of(core * hent + c * rows, rows), rows)

    def mate_block_of(c):
        return pl.ds(pl.multiple_of((1 - core) * hent + c * rows, rows), rows)

    def gather_src(step):
        out = []
        for j in list(range(1, chips)):
            c = pltpu.make_async_remote_copy(
                own_s.at[step], full_s.at[step, my_rows], ags_send.at[step, j], ags_recv.at[step, chip],
                device_id=(dom, peer(j) * 2 + core), device_id_type=MESH)
            c.start()
            out.append(c)
        c = pltpu.make_async_remote_copy(
            own_s.at[step], full_s.at[step, my_rows], fws_send.at[step, chip], fws_recv.at[step, chip],
            device_id=(dom, mate), device_id_type=MESH)
        c.start()
        out.append(c)
        full_s[step, my_rows] = own_s[step]
        return out

    def gather_dst(step):
        out = []
        for j in range(chips):
            c = pltpu.make_async_remote_copy(
                own_d.at[step], full_d.at[step, my_rows], agd_send.at[step, j], agd_recv.at[step, chip],
                device_id=(at_dom(step + 1), peer(j) * 2 + core), device_id_type=MESH)
            c.start()
            out.append(c)
        return out

    def forward(step, full, recv, fsend, frecv, first):
        out = []
        for j in range(first, chips):
            c = peer(j)
            blk = full.at[step, block_of(c)]
            pltpu.make_async_copy(blk, blk, recv.at[step, c]).wait()
            f = pltpu.make_async_remote_copy(
                blk, blk, fsend.at[step, c], frecv.at[step, c], device_id=(dom, mate), device_id_type=MESH)
            f.start()
            out.append(f)
        return out

    def from_mate(step, full, frecv):
        for c in range(chips):
            blk = full.at[step, mate_block_of(c)]
            pltpu.make_async_copy(blk, blk, frecv.at[step, c]).wait()

    def place(x):
        per = rows * 2
        return lax.rem(lax.div(x, rows), 2) * hent + lax.div(x, per) * rows + lax.rem(x, rows)

    def prepare(step):
        raw[pl.ds(edges // 8 * 8, ep - edges // 8 * 8)] = jnp.zeros((ep - edges // 8 * 8, wide), F32)
        unroll = 20

        def body(b, carry):
            for u in range(unroll):
                e = b * unroll + u
                i = er_ref[step, e]
                raw[pl.ds(e, 1), 0:width] = rel_v[pl.ds(i, 1), :]
            return carry

        lax.fori_loop(0, edges // unroll, body, 0)
        for m in range(0, ep, 128):
            x = raw[m:m + 128]
            ln = lax.broadcasted_iota(jnp.int32, (128, wide), 1)
            im = pltpu.roll(x, shift, axis=1)
            rsp[step, m:m + 128] = jnp.where(ln < half, x, jnp.where((ln >= hp) & (ln < hp + half), im, 0.0))

        def hots(ref, slot):
            ids[slot] = jnp.full((1, ep), -1, jnp.int32)
            ids[slot, :, 0:edges] = ref[step:step + 1, :]
            x = ids[slot]
            x = jnp.where(x < 0, -1, place(jnp.maximum(x, 0)))
            return x

        xs, xd, xn = hots(es_ref, 0), hots(ed_ref, 1), hots(ng_ref, 2)
        for m in range(0, ents, 128):
            line = lax.broadcasted_iota(jnp.int32, (128, ep), 0) + m
            s = jnp.where(line == xs, 1.0, 0.0)
            hot_t[step, m:m + 128] = s.astype(BF)
            hot[step, :, m:m + 128] = s.T.astype(BF)
            d = jnp.where(line == xd, 1.0, 0.0)
            c = jnp.sum(jnp.where(line == xn, 1.0, 0.0), axis=1, keepdims=True)
            pos[step, m:m + 128] = d
            wgt[step, m:m + 128] = d + c

    def split_to(ref, step, a, b):
        for m in range(0, ents, 128):
            a[m:m + 128], b[m:m + 128] = halves(ref[step, m:m + 128])

    def rotated(step):
        split_to(full_s, step, th, tl)
        for m in range(0, ep, 128):
            o = hot[step, m:m + 128]
            s = nn(o, th[...]) + nn(o, tl[...])
            sr, si = s[:, :hp], s[:, hp:]
            rr, ri = rsp[step, m:m + 128, :hp], rsp[step, m:m + 128, hp:]
            qh[m:m + 128, :hp], ql[m:m + 128, :hp] = halves(sr * rr - si * ri)
            qh[m:m + 128, hp:], ql[m:m + 128, hp:] = halves(sr * ri + si * rr)

    def weights(step):
        split_to(full_d, step, dh, dl)
        for m in range(0, ents, 128):
            a, b = dh[m:m + 128], dl[m:m + 128]
            s = nt(a, qh[...]) + (nt(a, ql[...]) + nt(b, qh[...]))
            w = jax.nn.sigmoid(s) * wgt[step, m:m + 128] - pos[step, m:m + 128]
            wth[m:m + 128], wtl[m:m + 128] = halves(w)
            wh[:, m:m + 128], wl[:, m:m + 128] = halves(w.T)

    lower = pl.ds(pl.multiple_of(core * hent, hent), hent)
    upper = pl.ds(pl.multiple_of((1 - core) * hent, hent), hent)

    def dst_part(which):
        a, b = wth[which], wtl[which]
        return nn(a, qh[...]) + (nn(a, ql[...]) + nn(b, qh[...]))

    def edge_grads(step):
        for m in range(0, ep, 128):
            a, b = wh[m:m + 128], wl[m:m + 128]
            g = nn(a, dh[...]) + (nn(a, dl[...]) + nn(b, dh[...]))
            gr, gi = g[:, :hp], g[:, hp:]
            rr, ri = rsp[step, m:m + 128, :hp], rsp[step, m:m + 128, hp:]
            qh[m:m + 128, :hp], ql[m:m + 128, :hp] = halves(gr * rr + gi * ri)
            qh[m:m + 128, hp:], ql[m:m + 128, hp:] = halves(gi * rr - gr * ri)

    def src_part(step, which):
        o = hot_t[step, which]
        return nn(o, qh[...]) + nn(o, ql[...])

    def to_mate(step, t, part, sib):
        c = pltpu.make_async_remote_copy(
            part.at[step], sib.at[step], dd_send.at[step, t], dd_recv.at[step, t],
            device_id=(dom, mate), device_id_type=MESH)
        c.start()
        return c

    def to_owners(step, t, copy, mine, sib, total, red, send, recv, target, first):
        copy.wait_recv()
        total[step] = mine + sib[step]
        out = []
        for j in range(first, chips):
            c = peer(j)
            r = pltpu.make_async_remote_copy(
                total.at[step, pl.ds(pl.multiple_of(c * rows, rows), rows)], red.at[step, chip],
                send.at[step, j], recv.at[step, chip],
                device_id=(target, c * 2 + core), device_id_type=MESH)
            r.start()
            out.append(r)
        if first == 1:
            red[step, chip] = total[step, pl.ds(pl.multiple_of(chip * rows, rows), rows)]
        return out

    def arrived(step, red, recv, first):
        for j in range(first, chips):
            blk = red.at[step, peer(j)]
            pltpu.make_async_copy(blk, blk, recv.at[step, peer(j)]).wait()
        g = red[step, 0]
        for c in range(1, chips):
            g = g + red[step, c]
        return g

    def adagrad(table, state, g):
        state = state + jnp.sum(g * g, axis=1, keepdims=True) / width
        return table - LEARN_RATE * g / (jnp.sqrt(state) + EPSILON), state

    pl.semaphore_wait(bar, count)

    sent = []
    sent += gather_src(0)
    sent += gather_dst(0)
    for c in rel_copies:
        c.wait()
    raw[...] = jnp.zeros((ep, wide), F32)
    prepare(0)

    for step in range(2):
        sent += forward(step, full_s, ags_recv, fws_send, fws_recv, 1)
        sent += forward(step, full_d, agd_recv, fwd_send, fwd_recv, 0)
        from_mate(step, full_s, fws_recv)
        rotated(step)
        from_mate(step, full_d, fwd_recv)
        weights(step)
        part_d[step] = dst_part(upper)
        cd = to_mate(step, 0, part_d, sib_d)
        mine_d = dst_part(lower)
        sent += to_owners(step, 0, cd, mine_d, sib_d, sum_d, red_d, rsd_send, rsd_recv, at_dom(-step - 1), 0)
        edge_grads(step)
        part_s[step] = src_part(step, upper)
        cs = to_mate(step, 1, part_s, sib_s)
        mine_s = src_part(step, lower)
        sent += to_owners(step, 1, cs, mine_s, sib_s, sum_s, red_s, rss_send, rss_recv, dom, 1)
        if step == 0:
            prepare(1)
        g = arrived(step, red_d, rsd_recv, 0)
        table, dst_state = adagrad(own_d[step], dst_state, g)
        if step == 0:
            own_d[1] = table
            sent += gather_dst(1)
        else:
            dst_out[...] = joined(table)
            dstt_out[...] = as_row(dst_state)
        g = arrived(step, red_s, rss_recv, 1)
        table, src_state = adagrad(own_s[step], src_state, g)
        if step == 0:
            own_s[1] = table
            sent += gather_src(1)
        else:
            src_out[...] = joined(table)
            sst_out[...] = as_row(src_state)
        sent += [cd, cs]
    for c in sent:
        c.wait_send()


def solution(mesh):
    doms, edge_axis = mesh.shape["dom"], mesh.shape["edge"]
    chips = edge_axis // 2

    def on_device(
        src_table, src_state, dst_table, dst_state, relations, edge_src, edge_rel, edge_dst, negatives
    ):
        rows, width = src_table.shape
        half = width // 2
        wide = 2 * up(half, 128)
        ents = rows * edge_axis
        edges = edge_src.shape[1]
        ep = up(edges, 128)
        nrel = relations.shape[0]
        vm, dma = pltpu.VMEM, pltpu.SemaphoreType.DMA
        in_vmem = pl.BlockSpec(memory_space=pltpu.VMEM)
        shard = jax.ShapeDtypeStruct((rows, width), F32)
        line = jax.ShapeDtypeStruct((1, rows), F32)
        out = pl.pallas_call(
            functools.partial(kernel, doms, chips, half),
            out_shape=(shard, line, shard, line),
            in_specs=[in_vmem] * 4
            + [pl.BlockSpec(memory_space=pl.ANY), in_vmem, pl.BlockSpec(memory_space=pltpu.SMEM)]
            + [in_vmem] * 2,
            out_specs=(in_vmem,) * 4,
            scratch_shapes=[
                vm((nrel, width), F32),
                vm((ep, wide), F32),
                vm((2, ep, wide), F32),
                vm((2, ep, ents), BF),
                vm((2, ents, ep), BF),
                vm((2, ents, ep), F32),
                vm((2, ents, ep), F32),
                vm((3, 1, ep), jnp.int32),
            ]
            + [vm((2, rows, wide), F32)] * 2
            + [vm((2, ents, wide), F32)] * 2
            + [vm((2, ents // 2, wide), F32)] * 6
            + [vm((2, chips, rows, wide), F32)] * 2
            + [vm((ep, wide), BF)] * 2
            + [vm((ents, wide), BF)] * 4
            + [vm((ents, ep), BF)] * 2
            + [vm((ep, ents), BF)] * 2
            + [dma((8,))]
            + [dma((2, chips))] * 8
            + [dma((2, 2))] * 2
            + [dma((2, chips))] * 4,
            compiler_params=pltpu.CompilerParams(
                collective_id=0, has_side_effects=True, vmem_limit_bytes=60 * 1024 * 1024
            ),
        )(
            src_table,
            src_state.reshape(1, rows),
            dst_table,
            dst_state.reshape(1, rows),
            relations,
            edge_src,
            edge_rel,
            edge_dst,
            negatives.reshape(2, edges),
        )
        return out[0], out[1].reshape(rows), out[2], out[3].reshape(rows)

    return jax.shard_map(
        on_device,
        mesh=mesh,
        in_specs=(
            P(("dom", "edge"), None),
            P(("dom", "edge")),
            P(("dom", "edge"), None),
            P(("dom", "edge")),
            P(),
            P(None, ("dom", "edge")),
            P(None, ("dom", "edge")),
            P(None, ("dom", "edge")),
            P(None, ("dom", "edge"), None),
        ),
        out_specs=(
            P(("dom", "edge"), None),
            P(("dom", "edge")),
            P(("dom", "edge"), None),
            P(("dom", "edge")),
        ),
        check_vma=False,
    )
```

```python
import functools

import jax
import jax.numpy as jnp
from jax import lax
from jax.experimental import pallas as pl
from jax.experimental.pallas import tpu as pltpu
from jax.sharding import PartitionSpec as P

MESH = pl.DeviceIdType.MESH
LEARN_RATE = 0.1
EPSILON = 1e-06
BF = jnp.bfloat16
F32 = jnp.float32


def up(n, m):
    return (n + m - 1) // m * m


def halves(x):
    hi = x.astype(BF)
    return hi, (x - hi.astype(F32)).astype(BF)


def nn(a, b):
    return jnp.dot(a, b, preferred_element_type=F32)


def nt(a, b):
    return lax.dot_general(a, b, (((1,), (1,)), ((), ())), preferred_element_type=F32)


def kernel(
    doms, chips, half,
    src_ref, sst_ref, dst_ref, dstt_ref, rel_hbm, es_ref, er_ref, ed_ref, ng_ref,
    out_ref,
    rel_t, rel_e, rel_v, rsp, hot, hot_t, wgt, pos, ids,
    own_s, own_d, full_s, full_d, part_s, part_d, sib_s, sib_d, sum_s, sum_d, red_s, red_d,
    qh, ql, dh, dl, th, tl, wth, wtl, wh, wl,
    rel_sem, ags_send, ags_recv, agd_send, agd_recv, fws_send, fws_recv, fwd_send, fwd_recv,
    dd_send, dd_recv, rss_send, rss_recv, rsd_send, rsd_recv,
):
    rows = src_ref.shape[0]
    width = src_ref.shape[1]
    hp = up(half, 128)
    wide = 2 * hp
    ents = full_s.shape[1]
    hent = ents // 2
    edges = es_ref.shape[1]
    ep = rsp.shape[1]
    nrel = rel_hbm.shape[1]
    shift = hp - half

    dom = lax.axis_index("dom")
    k = lax.axis_index("edge")
    core = lax.rem(k, 2)
    chip = lax.div(k, 2)
    mate = chip * 2 + (1 - core)

    def at_dom(step):
        return lax.rem(dom + step + doms, doms)

    def peer(j):
        return lax.rem(chip + j, chips)

    piece = up(-(-width // rel_sem.shape[0]), 8)
    rel_copies = []
    for n in range(rel_sem.shape[0]):
        lo = n * piece
        size = min(piece, width - lo)
        if size > 0:
            c = pltpu.make_async_copy(
                rel_hbm.at[pl.ds(lo, size)], rel_t.at[pl.ds(lo, size)], rel_sem.at[n])
            c.start()
            rel_copies.append(c)

    bar = pltpu.get_barrier_semaphore()
    count = 1
    pl.semaphore_signal(bar, inc=1, device_id=(dom, mate), device_id_type=MESH)
    for j in range(1, chips):
        pl.semaphore_signal(bar, inc=1, device_id=(dom, peer(j) * 2 + core), device_id_type=MESH)
        count += 1
    for other in (at_dom(1), at_dom(-1)):
        for j in range(chips):
            pl.semaphore_signal(bar, inc=1, device_id=(other, peer(j) * 2 + core), device_id_type=MESH)
            count += 1

    lane = lax.broadcasted_iota(jnp.int32, (rows, wide), 1)

    def spread(x_ref, to):
        to[0] = jnp.zeros((rows, wide), F32)
        to[0, :, 0:width] = x_ref[...]
        x = to[0]
        im = pltpu.roll(x, shift, axis=1)
        to[0] = jnp.where(lane < half, x, jnp.where(lane >= hp, im, 0.0))

    spread(src_ref, own_s)
    spread(dst_ref, own_d)

    eye = lax.broadcasted_iota(jnp.int32, (rows, rows), 0) == lax.broadcasted_iota(jnp.int32, (rows, rows), 1)

    def column(x_ref):
        return jnp.sum(jnp.where(eye, jnp.broadcast_to(x_ref[...], (rows, rows)), 0.0), axis=1, keepdims=True)

    def as_row(x):
        return jnp.sum(jnp.where(eye, jnp.broadcast_to(x, (rows, rows)), 0.0), axis=0, keepdims=True)

    src_state = column(sst_ref)
    dst_state = column(dstt_ref)

    my_rows = pl.ds(pl.multiple_of(core * hent + chip * rows, rows), rows)

    def block_of(c):
        return pl.ds(pl.multiple_of(core * hent + c * rows, rows), rows)

    def mate_block_of(c):
        return pl.ds(pl.multiple_of((1 - core) * hent + c * rows, rows), rows)

    def gather_src(step):
        out = []
        for j in list(range(1, chips)):
            c = pltpu.make_async_remote_copy(
                own_s.at[step], full_s.at[step, my_rows], ags_send.at[step, j], ags_recv.at[step, chip],
                device_id=(dom, peer(j) * 2 + core), device_id_type=MESH)
            c.start()
            out.append(c)
        c = pltpu.make_async_remote_copy(
            own_s.at[step], full_s.at[step, my_rows], fws_send.at[step, chip], fws_recv.at[step, chip],
            device_id=(dom, mate), device_id_type=MESH)
        c.start()
        out.append(c)
        full_s[step, my_rows] = own_s[step]
        return out

    def gather_dst(step):
        out = []
        for j in range(chips):
            c = pltpu.make_async_remote_copy(
                own_d.at[step], full_d.at[step, my_rows], agd_send.at[step, j], agd_recv.at[step, chip],
                device_id=(at_dom(step + 1), peer(j) * 2 + core), device_id_type=MESH)
            c.start()
            out.append(c)
        return out

    def forward(step, full, recv, fsend, frecv, first):
        out = []
        for j in range(first, chips):
            c = peer(j)
            blk = full.at[step, block_of(c)]
            pltpu.make_async_copy(blk, blk, recv.at[step, c]).wait()
            f = pltpu.make_async_remote_copy(
                blk, blk, fsend.at[step, c], frecv.at[step, c], device_id=(dom, mate), device_id_type=MESH)
            f.start()
            out.append(f)
        return out

    def from_mate(step, full, frecv):
        for c in range(chips):
            blk = full.at[step, mate_block_of(c)]
            pltpu.make_async_copy(blk, blk, frecv.at[step, c]).wait()

    def place(x):
        per = rows * 2
        return lax.rem(lax.div(x, rows), 2) * hent + lax.div(x, per) * rows + lax.rem(x, rows)

    def turn_relations():
        fill = jnp.zeros((hp - half, 128), F32)
        full = nrel // 128

        def turned(ref, cols, to):
            rel_v[to, 0:hp] = jnp.concatenate([ref[0:half, cols], fill], axis=0).T
            rel_v[to, hp:wide] = jnp.concatenate([ref[half:width, cols], fill], axis=0).T

        def body(b, carry):
            cols = pl.ds(pl.multiple_of(b * 128, 128), 128)
            turned(rel_t, cols, cols)
            return carry

        lax.fori_loop(0, full, body, 0)
        if nrel % 128:
            rel_e[...] = jnp.zeros((width, 128), F32)
            rel_e[:, 0:nrel % 128] = rel_t[:, full * 128:nrel]
            turned(rel_e, slice(0, 128), slice(full * 128, full * 128 + 128))

    def prepare(step):
        tail = edges // 8 * 8
        rsp[step, tail:ep] = jnp.zeros((ep - tail, wide), F32)
        unroll = 20

        def body(b, carry):
            for u in range(unroll):
                e = b * unroll + u
                i = er_ref[step, e]
                rsp[step, pl.ds(e, 1), :] = rel_v[pl.ds(i, 1), :]
            return carry

        lax.fori_loop(0, edges // unroll, body, 0)

        def hots(ref, slot):
            ids[slot] = jnp.full((1, ep), -1, jnp.int32)
            ids[slot, :, 0:edges] = ref[step] if len(ref.shape) == 3 else ref[step:step + 1, :]
            x = ids[slot]
            x = jnp.where(x < 0, -1, place(jnp.maximum(x, 0)))
            return x

        xs, xd, xn = hots(es_ref, 0), hots(ed_ref, 1), hots(ng_ref, 2)
        for m in range(0, ents, 128):
            line = lax.broadcasted_iota(jnp.int32, (128, ep), 0) + m
            s = jnp.where(line == xs, 1.0, 0.0)
            hot_t[step, m:m + 128] = s.astype(BF)
            hot[step, :, m:m + 128] = s.T.astype(BF)
            d = jnp.where(line == xd, 1.0, 0.0)
            c = jnp.sum(jnp.where(line == xn, 1.0, 0.0), axis=1, keepdims=True)
            pos[step, m:m + 128] = d
            wgt[step, m:m + 128] = d + c

    def split_to(ref, step, a, b):
        for m in range(0, ents, 128):
            a[m:m + 128], b[m:m + 128] = halves(ref[step, m:m + 128])

    def rotated(step):
        split_to(full_s, step, th, tl)
        for m in range(0, ep, 128):
            o = hot[step, m:m + 128]
            s = nn(o, th[...]) + nn(o, tl[...])
            sr, si = s[:, :hp], s[:, hp:]
            rr, ri = rsp[step, m:m + 128, :hp], rsp[step, m:m + 128, hp:]
            qh[m:m + 128, :hp], ql[m:m + 128, :hp] = halves(sr * rr - si * ri)
            qh[m:m + 128, hp:], ql[m:m + 128, hp:] = halves(sr * ri + si * rr)

    def weights(step):
        split_to(full_d, step, dh, dl)
        for m in range(0, ents, 128):
            a, b = dh[m:m + 128], dl[m:m + 128]
            s = nt(a, qh[...]) + (nt(a, ql[...]) + nt(b, qh[...]))
            w = jax.nn.sigmoid(s) * wgt[step, m:m + 128] - pos[step, m:m + 128]
            wth[m:m + 128], wtl[m:m + 128] = halves(w)
            wh[:, m:m + 128], wl[:, m:m + 128] = halves(w.T)

    lower = pl.ds(pl.multiple_of(core * hent, hent), hent)
    upper = pl.ds(pl.multiple_of((1 - core) * hent, hent), hent)

    def dst_part(which):
        a, b = wth[which], wtl[which]
        return nn(a, qh[...]) + (nn(a, ql[...]) + nn(b, qh[...]))

    def edge_grads(step):
        for m in range(0, ep, 128):
            a, b = wh[m:m + 128], wl[m:m + 128]
            g = nn(a, dh[...]) + (nn(a, dl[...]) + nn(b, dh[...]))
            gr, gi = g[:, :hp], g[:, hp:]
            rr, ri = rsp[step, m:m + 128, :hp], rsp[step, m:m + 128, hp:]
            qh[m:m + 128, :hp], ql[m:m + 128, :hp] = halves(gr * rr + gi * ri)
            qh[m:m + 128, hp:], ql[m:m + 128, hp:] = halves(gi * rr - gr * ri)

    def src_part(step, which):
        o = hot_t[step, which]
        return nn(o, qh[...]) + nn(o, ql[...])

    def to_mate(step, t, part, sib):
        c = pltpu.make_async_remote_copy(
            part.at[step], sib.at[step], dd_send.at[step, t], dd_recv.at[step, t],
            device_id=(dom, mate), device_id_type=MESH)
        c.start()
        return c

    def to_owners(step, t, copy, mine, sib, total, red, send, recv, target, first):
        copy.wait_recv()
        total[step] = mine + sib[step]
        out = []
        for j in range(first, chips):
            c = peer(j)
            r = pltpu.make_async_remote_copy(
                total.at[step, pl.ds(pl.multiple_of(c * rows, rows), rows)], red.at[step, chip],
                send.at[step, j], recv.at[step, chip],
                device_id=(target, c * 2 + core), device_id_type=MESH)
            r.start()
            out.append(r)
        if first == 1:
            red[step, chip] = total[step, pl.ds(pl.multiple_of(chip * rows, rows), rows)]
        return out

    def arrived(step, red, recv, first):
        for j in range(first, chips):
            blk = red.at[step, peer(j)]
            pltpu.make_async_copy(blk, blk, recv.at[step, peer(j)]).wait()
        g = red[step, 0]
        for c in range(1, chips):
            g = g + red[step, c]
        return g

    def adagrad(table, state, g):
        state = state + jnp.sum(g * g, axis=1, keepdims=True) / width
        return table - LEARN_RATE * g / (jnp.sqrt(state) + EPSILON), state

    pl.semaphore_wait(bar, count)

    sent = []
    sent += gather_src(0)
    sent += gather_dst(0)
    for c in rel_copies:
        c.wait()
    turn_relations()
    prepare(0)

    for step in range(2):
        sent += forward(step, full_s, ags_recv, fws_send, fws_recv, 1)
        sent += forward(step, full_d, agd_recv, fwd_send, fwd_recv, 0)
        from_mate(step, full_s, fws_recv)
        rotated(step)
        from_mate(step, full_d, fwd_recv)
        weights(step)
        part_d[step] = dst_part(upper)
        cd = to_mate(step, 0, part_d, sib_d)
        mine_d = dst_part(lower)
        sent += to_owners(step, 0, cd, mine_d, sib_d, sum_d, red_d, rsd_send, rsd_recv, at_dom(-step - 1), 0)
        edge_grads(step)
        part_s[step] = src_part(step, upper)
        cs = to_mate(step, 1, part_s, sib_s)
        mine_s = src_part(step, lower)
        sent += to_owners(step, 1, cs, mine_s, sib_s, sum_s, red_s, rss_send, rss_recv, dom, 1)
        if step == 0:
            prepare(1)
        g = arrived(step, red_d, rsd_recv, 0)
        table, dst_state = adagrad(own_d[step], dst_state, g)
        if step == 0:
            own_d[1] = table
            sent += gather_dst(1)
        else:
            out_ref[rows:2 * rows] = table
            out_ref[2 * rows + 1:2 * rows + 2, 0:rows] = as_row(dst_state)
        g = arrived(step, red_s, rss_recv, 1)
        table, src_state = adagrad(own_s[step], src_state, g)
        if step == 0:
            own_s[1] = table
            sent += gather_src(1)
        else:
            out_ref[0:rows] = table
            out_ref[2 * rows:2 * rows + 1, 0:rows] = as_row(src_state)
        sent += [cd, cs]
    for c in sent:
        c.wait_send()


def finish(half, res_ref, src_out, sst_out, dst_out, dstt_out):
    rows, width = src_out.shape
    wide = res_ref.shape[1]
    lane = lax.broadcasted_iota(jnp.int32, (rows, wide), 1)
    for first, out in ((0, src_out), (rows, dst_out)):
        x = res_ref[first:first + rows]
        im = pltpu.roll(x, wide // 2 + half, axis=1)
        out[...] = jnp.where(lane < half, x, im)[:, :width]
    sst_out[...] = res_ref[2 * rows:2 * rows + 1, 0:rows]
    dstt_out[...] = res_ref[2 * rows + 1:2 * rows + 2, 0:rows]


def solution(mesh):
    doms, edge_axis = mesh.shape["dom"], mesh.shape["edge"]
    chips = edge_axis // 2

    def on_device(
        src_table, src_state, dst_table, dst_state, relations, edge_src, edge_rel, edge_dst, negatives
    ):
        rows, width = src_table.shape
        half = width // 2
        wide = 2 * up(half, 128)
        ents = rows * edge_axis
        edges = edge_src.shape[1]
        ep = up(edges, 128)
        nrel = relations.shape[0]
        vm, dma = pltpu.VMEM, pltpu.SemaphoreType.DMA
        in_vmem = pl.BlockSpec(memory_space=pltpu.VMEM)
        shard = jax.ShapeDtypeStruct((rows, width), F32)
        line = jax.ShapeDtypeStruct((1, rows), F32)
        packed = pl.pallas_call(
            functools.partial(kernel, doms, chips, half),
            out_shape=jax.ShapeDtypeStruct((2 * rows + 8, wide), F32),
            in_specs=[in_vmem] * 4
            + [pl.BlockSpec(memory_space=pl.ANY), in_vmem, pl.BlockSpec(memory_space=pltpu.SMEM)]
            + [in_vmem] * 2,
            out_specs=in_vmem,
            scratch_shapes=[
                vm((width, nrel), F32),
                vm((width, 128), F32),
                vm((up(nrel, 128), wide), F32),
                vm((2, ep, wide), F32),
                vm((2, ep, ents), BF),
                vm((2, ents, ep), BF),
                vm((2, ents, ep), F32),
                vm((2, ents, ep), F32),
                vm((3, 1, ep), jnp.int32),
            ]
            + [vm((2, rows, wide), F32)] * 2
            + [vm((2, ents, wide), F32)] * 2
            + [vm((2, ents // 2, wide), F32)] * 6
            + [vm((2, chips, rows, wide), F32)] * 2
            + [vm((ep, wide), BF)] * 2
            + [vm((ents, wide), BF)] * 4
            + [vm((ents, ep), BF)] * 2
            + [vm((ep, ents), BF)] * 2
            + [dma((8,))]
            + [dma((2, chips))] * 8
            + [dma((2, 2))] * 2
            + [dma((2, chips))] * 4,
            compiler_params=pltpu.CompilerParams(
                collective_id=0, has_side_effects=True, vmem_limit_bytes=60 * 1024 * 1024
            ),
        )(
            src_table,
            src_state.reshape(1, rows),
            dst_table,
            dst_state.reshape(1, rows),
            relations.T,
            edge_src,
            edge_rel,
            edge_dst,
            negatives,
        )
        out = pl.pallas_call(
            functools.partial(finish, half),
            out_shape=(shard, line, shard, line),
            in_specs=[in_vmem],
            out_specs=(in_vmem,) * 4,
        )(packed)
        return out[0], out[1].reshape(rows), out[2], out[3].reshape(rows)

    return jax.shard_map(
        on_device,
        mesh=mesh,
        in_specs=(
            P(("dom", "edge"), None),
            P(("dom", "edge")),
            P(("dom", "edge"), None),
            P(("dom", "edge")),
            P(),
            P(None, ("dom", "edge")),
            P(None, ("dom", "edge")),
            P(None, ("dom", "edge")),
            P(None, ("dom", "edge"), None),
        ),
        out_specs=(
            P(("dom", "edge"), None),
            P(("dom", "edge")),
            P(("dom", "edge"), None),
            P(("dom", "edge")),
        ),
        check_vma=False,
    )
```

```python
import functools

import jax
import jax.numpy as jnp
from jax import lax
from jax.experimental import pallas as pl
from jax.experimental.pallas import tpu as pltpu
from jax.sharding import PartitionSpec as P

MESH = pl.DeviceIdType.MESH
LEARN_RATE = 0.1
EPSILON = 1e-06
MSG = 50
BF = jnp.bfloat16
F32 = jnp.float32


def up(n, m):
    return (n + m - 1) // m * m


def halves(x):
    hi = x.astype(BF)
    return hi, (x - hi.astype(F32)).astype(BF)


def nn(a, b):
    return jnp.dot(a, b, preferred_element_type=F32)


def nt(a, b):
    return lax.dot_general(a, b, (((1,), (1,)), ((), ())), preferred_element_type=F32)


def lanes(n):
    return lax.broadcasted_iota(jnp.int32, (n, 128), 1)


def packed_rows(x):
    a0, a1, b0, b1 = (x[:, n * 128:(n + 1) * 128] for n in range(4))
    lane = lanes(x.shape[0])
    both = jnp.where(lane < 64, a1, pltpu.roll(b1, 64, axis=1))
    left = jnp.where(lane < 8, pltpu.roll(a1, 64, axis=1), jnp.where(lane < 16, pltpu.roll(b1, 72, axis=1), 0.0))
    for n in (16, 32, 64):
        left = left + pltpu.roll(left, n, axis=1)
    line = lax.rem(lax.broadcasted_iota(jnp.int32, lane.shape, 0), 8)
    left = jnp.where(lax.div(lane, 16) == 7 - line, left, 0.0)
    tails = [jnp.sum(left[t:t + 8], axis=0, keepdims=True) for t in range(0, x.shape[0], 8)]
    return a0, b0, both, tails


def put_packed(ref, x):
    a0, b0, both, tails = packed_rows(x)
    n = x.shape[0]
    ref[0:n] = a0
    ref[n:2 * n] = b0
    ref[2 * n:3 * n] = both
    for t, row in enumerate(tails):
        ref[3 * n + t:3 * n + t + 1] = row


def unpacked(x, tails):
    n = x.shape[0] // 3
    lane = lanes(n)
    a0, b0, both = x[0:n], x[n:2 * n], x[2 * n:3 * n]
    re = []
    for row in tails:
        v = jnp.broadcast_to(pltpu.roll(row, 80, axis=1), (8, 128))
        re.append(pltpu.roll(v, 0, axis=1, stride=16, stride_axis=0))
    re = jnp.concatenate(re, axis=0)
    im = pltpu.roll(re, 120, axis=1)
    a1 = jnp.where(lane < 64, both, jnp.where(lane < 72, re, 0.0))
    b1 = jnp.where(lane < 64, pltpu.roll(both, 64, axis=1), jnp.where(lane < 72, im, 0.0))
    return jnp.concatenate([a0, a1, b0, b1], axis=1)


def tail_rows(x_ref, n):
    return [x_ref[3 * n + t:3 * n + t + 1] for t in range(n // 8)]


def kernel(
    doms, chips, half,
    src_hbm, sst_hbm, dst_hbm, dstt_hbm, rel_hbm, es_hbm, er_hbm, ed_hbm, ng_hbm,
    out_ref,
    src_ref, sst_ref, dst_ref, dstt_ref, es_ref, er_ref, ed_ref, ng_ref,
    rel_t, rel_e, rel_v, rsp, hot, hot_t, wgt, pos, ids,
    tab_s, tab_d, own_s, own_d, full_s, full_d, part_s, part_d, sib_s, sib_d, sum_s, sum_d, red_s, red_d,
    qh, ql, dh, dl, th, tl, wth, wtl, wh, wl,
    in_sem, rel_sem, ags_send, ags_recv, agd_send, agd_recv, fws_send, fws_recv, fwd_send, fwd_recv,
    dd_send, dd_recv, rss_send, rss_recv, rsd_send, rsd_recv,
):
    rows, width = src_ref.shape
    hp = up(half, 128)
    wide = 2 * hp
    ents = th.shape[0]
    hent = ents // 2
    shards = rows // 16
    edges = es_ref.shape[1]
    ep = rsp.shape[1]
    nrel = rel_hbm.shape[1]
    shift = hp - half

    dom = lax.axis_index("dom")
    k = lax.axis_index("edge")
    core = lax.rem(k, 2)
    chip = lax.div(k, 2)
    mate = chip * 2 + (1 - core)
    nx = chips // 2

    def at_dom(step):
        return lax.rem(dom + step + doms, doms)

    def far(o):
        return min(o[0], nx - o[0]) + 2 * o[1]

    offsets = sorted(((dx, dy) for dx in range(nx) for dy in range(2)), key=lambda o: -far(o))
    others = [o for o in offsets if o != (0, 0)]

    def peer(o):
        return lax.rem(lax.div(chip, 2) + o[0], nx) * 2 + lax.rem(lax.rem(chip, 2) + o[1], 2)

    bar = pltpu.get_barrier_semaphore()
    count = 1
    for other in (at_dom(1), at_dom(-1)):
        for o in offsets:
            pl.semaphore_signal(bar, inc=1, device_id=(other, peer(o) * 2 + core), device_id_type=MESH)
            count += 1
    for o in others:
        pl.semaphore_signal(bar, inc=1, device_id=(dom, peer(o) * 2 + core), device_id_type=MESH)
        count += 1
    pl.semaphore_signal(bar, inc=1, device_id=(dom, mate), device_id_type=MESH)

    inputs = []
    for n, (a, b) in enumerate((
        (src_hbm, src_ref), (dst_hbm, dst_ref), (sst_hbm, sst_ref), (dstt_hbm, dstt_ref),
        (es_hbm, es_ref), (er_hbm, er_ref), (ed_hbm, ed_ref), (ng_hbm, ng_ref),
    )):
        c = pltpu.make_async_copy(a, b, in_sem.at[n])
        c.start()
        inputs.append(c)
    piece = up(-(-width // rel_sem.shape[0]), 8)
    rel_copies = []
    for n in range(rel_sem.shape[0]):
        lo = n * piece
        size = min(piece, width - lo)
        if size > 0:
            c = pltpu.make_async_copy(
                rel_hbm.at[pl.ds(lo, size)], rel_t.at[pl.ds(lo, size)], rel_sem.at[n])
            c.start()
            rel_copies.append(c)

    lane = lax.broadcasted_iota(jnp.int32, (rows, wide), 1)

    def put_table(step, table, tab, own):
        tab[step] = table
        for n in range(shards):
            put_packed(own.at[step, n], table[n * 16:n * 16 + 16])

    def spread(x_ref, tab, own):
        tab[0] = jnp.zeros((rows, wide), F32)
        tab[0, :, 0:width] = x_ref[...]
        x = tab[0]
        im = pltpu.roll(x, shift, axis=1)
        put_table(0, jnp.where(lane < half, x, jnp.where(lane >= hp, im, 0.0)), tab, own)

    for c in inputs:
        c.wait()
    spread(src_ref, tab_s, own_s)
    spread(dst_ref, tab_d, own_d)

    eye = lax.broadcasted_iota(jnp.int32, (rows, rows), 0) == lax.broadcasted_iota(jnp.int32, (rows, rows), 1)

    def column(x_ref):
        return jnp.sum(jnp.where(eye, jnp.broadcast_to(x_ref[...], (rows, rows)), 0.0), axis=1, keepdims=True)

    def as_row(x):
        return jnp.sum(jnp.where(eye, jnp.broadcast_to(x, (rows, rows)), 0.0), axis=0, keepdims=True)

    src_state = column(sst_ref)
    dst_state = column(dstt_ref)

    mine = core * chips + chip

    def gather_src(step):
        out = []
        for n, o in enumerate(others):
            c = pltpu.make_async_remote_copy(
                own_s.at[step], full_s.at[step, mine], ags_send.at[step, n], ags_recv.at[step, chip],
                device_id=(dom, peer(o) * 2 + core), device_id_type=MESH)
            c.start()
            out.append(c)
        c = pltpu.make_async_remote_copy(
            own_s.at[step], full_s.at[step, mine], fws_send.at[step, chip], fws_recv.at[step, chip],
            device_id=(dom, mate), device_id_type=MESH)
        c.start()
        out.append(c)
        full_s[step, mine] = own_s[step]
        return out

    def gather_dst(step):
        out = []
        for n, o in enumerate(offsets):
            c = pltpu.make_async_remote_copy(
                own_d.at[step], full_d.at[step, mine], agd_send.at[step, n], agd_recv.at[step, chip],
                device_id=(at_dom(step + 1), peer(o) * 2 + core), device_id_type=MESH)
            c.start()
            out.append(c)
        return out

    def forward(step, full, recv, fsend, frecv, which):
        out = []
        for o in reversed(which):
            c = peer(o)
            blk = full.at[step, core * chips + c]
            pltpu.make_async_copy(blk, blk, recv.at[step, c]).wait()
            f = pltpu.make_async_remote_copy(
                blk, blk, fsend.at[step, c], frecv.at[step, c], device_id=(dom, mate), device_id_type=MESH)
            f.start()
            out.append(f)
        return out

    def from_mate(step, full, frecv):
        for c in range(chips):
            blk = full.at[step, (1 - core) * chips + c]
            pltpu.make_async_copy(blk, blk, frecv.at[step, c]).wait()

    def place(x):
        per = rows * 2
        return lax.rem(lax.div(x, rows), 2) * hent + lax.div(x, per) * rows + lax.rem(x, rows)

    def turn_relations():
        fill = jnp.zeros((hp - half, 128), F32)
        full = nrel // 128

        def turned(ref, cols, to):
            rel_v[to, 0:hp] = jnp.concatenate([ref[0:half, cols], fill], axis=0).T
            rel_v[to, hp:wide] = jnp.concatenate([ref[half:width, cols], fill], axis=0).T

        def body(b, carry):
            cols = pl.ds(pl.multiple_of(b * 128, 128), 128)
            turned(rel_t, cols, cols)
            return carry

        lax.fori_loop(0, full, body, 0)
        if nrel % 128:
            rel_e[...] = jnp.zeros((width, 128), F32)
            rel_e[:, 0:nrel % 128] = rel_t[:, full * 128:nrel]
            turned(rel_e, slice(0, 128), slice(full * 128, full * 128 + 128))

    def prepare(step):
        tail = edges // 8 * 8
        rsp[step, tail:ep] = jnp.zeros((ep - tail, wide), F32)
        unroll = 20

        def body(b, carry):
            for u in range(unroll):
                e = b * unroll + u
                i = er_ref[step, e]
                rsp[step, pl.ds(e, 1), :] = rel_v[pl.ds(i, 1), :]
            return carry

        lax.fori_loop(0, edges // unroll, body, 0)

        def hots(ref, slot):
            ids[slot] = jnp.full((1, ep), -1, jnp.int32)
            ids[slot, :, 0:edges] = ref[step] if len(ref.shape) == 3 else ref[step:step + 1, :]
            x = ids[slot]
            return jnp.where(x < 0, -1, place(jnp.maximum(x, 0)))

        xs, xd, xn = hots(es_ref, 0), hots(ed_ref, 1), hots(ng_ref, 2)
        for m in range(0, ents, 128):
            line = lax.broadcasted_iota(jnp.int32, (128, ep), 0) + m
            s = jnp.where(line == xs, 1.0, 0.0)
            hot_t[step, m:m + 128] = s.astype(BF)
            hot[step, :, m:m + 128] = s.T.astype(BF)
            d = jnp.where(line == xd, 1.0, 0.0)
            c = jnp.sum(jnp.where(line == xn, 1.0, 0.0), axis=1, keepdims=True)
            pos[step, m:m + 128] = d
            wgt[step, m:m + 128] = d + c

    lower = pl.ds(pl.multiple_of(core * hent, hent), hent)
    upper = pl.ds(pl.multiple_of((1 - core) * hent, hent), hent)

    def split_to(full, step, side, a, b):
        for c in range(chips):
            for n in range(shards):
                blk = full.at[step, side * chips + c, n]
                at = pl.ds(pl.multiple_of(side * hent + c * rows + n * 16, 16), 16)
                a[at], b[at] = halves(unpacked(blk[0:48], tail_rows(blk, 16)))

    def rotated(step):
        for m in range(0, ep, 128):
            o = hot[step, m:m + 128]
            s = nn(o, th[...]) + nn(o, tl[...])
            sr, si = s[:, :hp], s[:, hp:]
            rr, ri = rsp[step, m:m + 128, :hp], rsp[step, m:m + 128, hp:]
            qh[m:m + 128, :hp], ql[m:m + 128, :hp] = halves(sr * rr - si * ri)
            qh[m:m + 128, hp:], ql[m:m + 128, hp:] = halves(sr * ri + si * rr)

    def weights(step, side):
        for m in range(0, hent, 128):
            at = pl.ds(pl.multiple_of(side * hent + m, 128), 128)
            a, b = dh[at], dl[at]
            s = nt(a, qh[...]) + (nt(a, ql[...]) + nt(b, qh[...]))
            w = jax.nn.sigmoid(s) * wgt[step, at] - pos[step, at]
            wth[at], wtl[at] = halves(w)
            wh[:, at], wl[:, at] = halves(w.T)

    def dst_part(which):
        a, b = wth[which], wtl[which]
        return nn(a, qh[...]) + (nn(a, ql[...]) + nn(b, qh[...]))

    def edge_grads(step):
        for m in range(0, ep, 128):
            a, b = wh[m:m + 128], wl[m:m + 128]
            g = nn(a, dh[...]) + (nn(a, dl[...]) + nn(b, dh[...]))
            gr, gi = g[:, :hp], g[:, hp:]
            rr, ri = rsp[step, m:m + 128, :hp], rsp[step, m:m + 128, hp:]
            qh[m:m + 128, :hp], ql[m:m + 128, :hp] = halves(gr * rr + gi * ri)
            qh[m:m + 128, hp:], ql[m:m + 128, hp:] = halves(gi * rr - gr * ri)

    def src_part(step, which):
        o = hot_t[step, which]
        return nn(o, qh[...]) + nn(o, ql[...])

    def to_mate(step, t, part, sib):
        c = pltpu.make_async_remote_copy(
            part.at[step], sib.at[step], dd_send.at[step, t], dd_recv.at[step, t],
            device_id=(dom, mate), device_id_type=MESH)
        c.start()
        return c

    def to_owners(step, copy, part, sib, total, red, send, recv, target, which):
        copy.wait_recv()
        for c in range(chips):
            for n in range(shards):
                at = slice(c * rows + n * 16, c * rows + n * 16 + 16)
                put_packed(total.at[step, c, n], part[at] + sib[step, at])
        out = []
        for n, o in enumerate(which):
            c = peer(o)
            r = pltpu.make_async_remote_copy(
                total.at[step, c], red.at[step, chip], send.at[step, n], recv.at[step, chip],
                device_id=(target, c * 2 + core), device_id_type=MESH)
            r.start()
            out.append(r)
        if len(which) < chips:
            red[step, chip] = total[step, chip]
        return out

    def arrived(step, red, recv, which):
        for o in reversed(which):
            blk = red.at[step, peer(o)]
            pltpu.make_async_copy(blk, blk, recv.at[step, peer(o)]).wait()
        out = []
        for n in range(shards):
            g, tails = red[step, 0, n, 0:48], tail_rows(red.at[step, 0, n], 16)
            for c in range(1, chips):
                g = g + red[step, c, n, 0:48]
                tails = [t + u for t, u in zip(tails, tail_rows(red.at[step, c, n], 16))]
            out.append(unpacked(g, tails))
        return out[0] if shards == 1 else jnp.concatenate(out, axis=0)

    def adagrad(table, state, g):
        state = state + jnp.sum(g * g, axis=1, keepdims=True) / width
        return table - LEARN_RATE * g / (jnp.sqrt(state) + EPSILON), state

    pl.semaphore_wait(bar, count)

    sent = []
    sent += gather_src(0)
    sent += gather_dst(0)
    for c in rel_copies:
        c.wait()
    turn_relations()
    prepare(0)

    for step in range(2):
        if step == 0:
            sent += forward(step, full_s, ags_recv, fws_send, fws_recv, others)
            sent += forward(step, full_d, agd_recv, fwd_send, fwd_recv, offsets)
        else:
            sent += forward(step, full_d, agd_recv, fwd_send, fwd_recv, offsets)
            sent += forward(step, full_s, ags_recv, fws_send, fws_recv, others)
        split_to(full_s, step, core, th, tl)
        from_mate(step, full_s, fws_recv)
        split_to(full_s, step, 1 - core, th, tl)
        rotated(step)
        split_to(full_d, step, core, dh, dl)
        weights(step, core)
        from_mate(step, full_d, fwd_recv)
        split_to(full_d, step, 1 - core, dh, dl)
        weights(step, 1 - core)
        part_d[step] = dst_part(upper)
        cd = to_mate(step, 0, part_d, sib_d)
        mine_d = dst_part(lower)
        sent += to_owners(step, cd, mine_d, sib_d, sum_d, red_d, rsd_send, rsd_recv, at_dom(-step - 1), offsets)
        edge_grads(step)
        part_s[step] = src_part(step, upper)
        cs = to_mate(step, 1, part_s, sib_s)
        mine_s = src_part(step, lower)
        sent += to_owners(step, cs, mine_s, sib_s, sum_s, red_s, rss_send, rss_recv, dom, others)
        if step == 0:
            prepare(1)
        g = arrived(step, red_d, rsd_recv, offsets)
        table, dst_state = adagrad(tab_d[step], dst_state, g)
        if step == 0:
            put_table(1, table, tab_d, own_d)
            sent += gather_dst(1)
        else:
            out_ref[rows:2 * rows] = table
            out_ref[2 * rows + 1:2 * rows + 2, 0:rows] = as_row(dst_state)
        g = arrived(step, red_s, rss_recv, others)
        table, src_state = adagrad(tab_s[step], src_state, g)
        if step == 0:
            put_table(1, table, tab_s, own_s)
            sent += gather_src(1)
        else:
            out_ref[0:rows] = table
            out_ref[2 * rows:2 * rows + 1, 0:rows] = as_row(src_state)
        sent += [cd, cs]
    for c in sent:
        c.wait_send()


def finish(half, res_ref, src_out, sst_out, dst_out, dstt_out):
    rows, width = src_out.shape
    wide = res_ref.shape[1]
    lane = lax.broadcasted_iota(jnp.int32, (rows, wide), 1)
    for first, out in ((0, src_out), (rows, dst_out)):
        x = res_ref[first:first + rows]
        im = pltpu.roll(x, wide // 2 + half, axis=1)
        out[...] = jnp.where(lane < half, x, im)[:, :width]
    sst_out[...] = res_ref[2 * rows:2 * rows + 1, 0:rows]
    dstt_out[...] = res_ref[2 * rows + 1:2 * rows + 2, 0:rows]


def solution(mesh):
    doms, edge_axis = mesh.shape["dom"], mesh.shape["edge"]
    chips = edge_axis // 2

    def on_device(
        src_table, src_state, dst_table, dst_state, relations, edge_src, edge_rel, edge_dst, negatives
    ):
        rows, width = src_table.shape
        half = width // 2
        wide = 2 * up(half, 128)
        ents = rows * edge_axis
        edges = edge_src.shape[1]
        ep = up(edges, 128)
        nrel = relations.shape[0]
        vm, dma = pltpu.VMEM, pltpu.SemaphoreType.DMA
        in_vmem = pl.BlockSpec(memory_space=pltpu.VMEM)
        in_hbm = pl.BlockSpec(memory_space=pltpu.HBM)
        shards = rows // 16
        block = (shards, MSG, 128)
        shard = jax.ShapeDtypeStruct((rows, width), F32)
        line = jax.ShapeDtypeStruct((1, rows), F32)
        packed = pl.pallas_call(
            functools.partial(kernel, doms, chips, half),
            out_shape=jax.ShapeDtypeStruct((2 * rows + 8, wide), F32),
            in_specs=[in_hbm] * 9,
            out_specs=in_vmem,
            scratch_shapes=[
                vm((rows, width), F32),
                vm((1, rows), F32),
                vm((rows, width), F32),
                vm((1, rows), F32),
                vm((2, edges), jnp.int32),
                pltpu.SMEM((2, edges), jnp.int32),
                vm((2, edges), jnp.int32),
                vm(negatives.shape, jnp.int32),
                vm((width, nrel), F32),
                vm((width, 128), F32),
                vm((up(nrel, 128), wide), F32),
                vm((2, ep, wide), F32),
                vm((2, ep, ents), BF),
                vm((2, ents, ep), BF),
                vm((2, ents, ep), F32),
                vm((2, ents, ep), F32),
                vm((3, 1, ep), jnp.int32),
            ]
            + [vm((2, rows, wide), F32)] * 2
            + [vm((2,) + block, F32)] * 2
            + [vm((2, edge_axis) + block, F32)] * 2
            + [vm((2, ents // 2, wide), F32)] * 4
            + [vm((2, chips) + block, F32)] * 4
            + [vm((ep, wide), BF)] * 2
            + [vm((ents, wide), BF)] * 4
            + [vm((ents, ep), BF)] * 2
            + [vm((ep, ents), BF)] * 2
            + [dma((8,))] * 2
            + [dma((2, chips))] * 8
            + [dma((2, 2))] * 2
            + [dma((2, chips))] * 4,
            compiler_params=pltpu.CompilerParams(
                collective_id=0, has_side_effects=True, vmem_limit_bytes=58 * 1024 * 1024
            ),
        )(
            src_table,
            src_state.reshape(1, rows),
            dst_table,
            dst_state.reshape(1, rows),
            relations.T,
            edge_src,
            edge_rel,
            edge_dst,
            negatives,
        )
        out = pl.pallas_call(
            functools.partial(finish, half),
            out_shape=(shard, line, shard, line),
            in_specs=[in_vmem],
            out_specs=(in_vmem,) * 4,
            compiler_params=pltpu.CompilerParams(vmem_limit_bytes=1024 * 1024),
        )(packed)
        return out[0], out[1].reshape(rows), out[2], out[3].reshape(rows)

    return jax.shard_map(
        on_device,
        mesh=mesh,
        in_specs=(
            P(("dom", "edge"), None),
            P(("dom", "edge")),
            P(("dom", "edge"), None),
            P(("dom", "edge")),
            P(),
            P(None, ("dom", "edge")),
            P(None, ("dom", "edge")),
            P(None, ("dom", "edge")),
            P(None, ("dom", "edge"), None),
        ),
        out_specs=(
            P(("dom", "edge"), None),
            P(("dom", "edge")),
            P(("dom", "edge"), None),
            P(("dom", "edge")),
        ),
        check_vma=False,
    )
```

```python
import functools

import jax
import jax.numpy as jnp
from jax import lax
from jax.experimental import pallas as pl
from jax.experimental.pallas import tpu as pltpu
from jax.sharding import PartitionSpec as P

MESH = pl.DeviceIdType.MESH
LEARN_RATE = 0.1
EPSILON = 1e-06
MSG = 50
BF = jnp.bfloat16
F32 = jnp.float32


def up(n, m):
    return (n + m - 1) // m * m


def halves(x):
    hi = x.astype(BF)
    return hi, (x - hi.astype(F32)).astype(BF)


def nn(a, b):
    return jnp.dot(a, b, preferred_element_type=F32)


def nt(a, b):
    return lax.dot_general(a, b, (((1,), (1,)), ((), ())), preferred_element_type=F32)


def lanes(n):
    return lax.broadcasted_iota(jnp.int32, (n, 128), 1)


def packed_rows(x):
    a0, a1, b0, b1 = (x[:, n * 128:(n + 1) * 128] for n in range(4))
    lane = lanes(x.shape[0])
    both = jnp.where(lane < 64, a1, pltpu.roll(b1, 64, axis=1))
    left = jnp.where(lane < 8, pltpu.roll(a1, 64, axis=1), jnp.where(lane < 16, pltpu.roll(b1, 72, axis=1), 0.0))
    for n in (16, 32, 64):
        left = left + pltpu.roll(left, n, axis=1)
    line = lax.rem(lax.broadcasted_iota(jnp.int32, lane.shape, 0), 8)
    left = jnp.where(lax.div(lane, 16) == 7 - line, left, 0.0)
    tails = [jnp.sum(left[t:t + 8], axis=0, keepdims=True) for t in range(0, x.shape[0], 8)]
    return a0, b0, both, tails


def put_packed(ref, x):
    a0, b0, both, tails = packed_rows(x)
    n = x.shape[0]
    ref[0:n] = a0
    ref[n:2 * n] = b0
    ref[2 * n:3 * n] = both
    for t, row in enumerate(tails):
        ref[3 * n + t:3 * n + t + 1] = row


def unpacked(x, tails):
    n = x.shape[0] // 3
    lane = lanes(n)
    a0, b0, both = x[0:n], x[n:2 * n], x[2 * n:3 * n]
    re = []
    for row in tails:
        v = jnp.broadcast_to(pltpu.roll(row, 80, axis=1), (8, 128))
        re.append(pltpu.roll(v, 0, axis=1, stride=16, stride_axis=0))
    re = jnp.concatenate(re, axis=0)
    im = pltpu.roll(re, 120, axis=1)
    a1 = jnp.where(lane < 64, both, jnp.where(lane < 72, re, 0.0))
    b1 = jnp.where(lane < 64, pltpu.roll(both, 64, axis=1), jnp.where(lane < 72, im, 0.0))
    return jnp.concatenate([a0, a1, b0, b1], axis=1)


def tail_rows(x_ref, n):
    return [x_ref[3 * n + t:3 * n + t + 1] for t in range(n // 8)]


def kernel(
    doms, chips, half,
    src_hbm, sst_hbm, dst_hbm, dstt_hbm, rel_hbm, es_hbm, er_hbm, ed_hbm, ng_hbm,
    out_ref,
    src_ref, sst_ref, dst_ref, dstt_ref, es_ref, er_ref, ed_ref, ng_ref,
    rel_t, rel_e, rel_v, rsp, hot, hot_t, wgt, pos, ids,
    tab_s, tab_d, own_s, own_d, full_s, full_d, part_s, part_d, sib_s, sib_d, sum_s, sum_d, red_s, red_d,
    qh, ql, dh, dl, th, tl, wth, wtl, wh, wl,
    in_sem, rel_sem, ags_send, ags_recv, agd_send, agd_recv, fws_send, fws_recv, fwd_send, fwd_recv,
    dd_send, dd_recv, rss_send, rss_recv, rsd_send, rsd_recv,
):
    rows, width = src_ref.shape
    hp = up(half, 128)
    wide = 2 * hp
    ents = th.shape[0]
    hent = ents // 2
    shards = rows // 16
    edges = es_ref.shape[1]
    ep = rsp.shape[1]
    nrel = rel_hbm.shape[1]
    shift = hp - half

    dom = lax.axis_index("dom")
    k = lax.axis_index("edge")
    core = lax.rem(k, 2)
    chip = lax.div(k, 2)
    mate = chip * 2 + (1 - core)
    nx = chips // 2

    def at_dom(step):
        return lax.rem(dom + step + doms, doms)

    def far(o):
        return min(o[0], nx - o[0]) + 2 * o[1]

    offsets = sorted(((dx, dy) for dx in range(nx) for dy in range(2)), key=lambda o: -far(o))
    others = [o for o in offsets if o != (0, 0)]

    def peer(o):
        return lax.rem(lax.div(chip, 2) + o[0], nx) * 2 + lax.rem(lax.rem(chip, 2) + o[1], 2)

    bar = pltpu.get_barrier_semaphore()
    count = 1
    for other in (at_dom(1), at_dom(-1)):
        for o in offsets:
            pl.semaphore_signal(bar, inc=1, device_id=(other, peer(o) * 2 + core), device_id_type=MESH)
            count += 1
    for o in others:
        pl.semaphore_signal(bar, inc=1, device_id=(dom, peer(o) * 2 + core), device_id_type=MESH)
        count += 1
    pl.semaphore_signal(bar, inc=1, device_id=(dom, mate), device_id_type=MESH)

    inputs = []
    for n, (a, b) in enumerate((
        (src_hbm, src_ref), (dst_hbm, dst_ref), (sst_hbm, sst_ref), (dstt_hbm, dstt_ref),
        (es_hbm, es_ref), (er_hbm, er_ref), (ed_hbm, ed_ref), (ng_hbm, ng_ref),
    )):
        c = pltpu.make_async_copy(a, b, in_sem.at[n])
        c.start()
        inputs.append(c)
    piece = up(-(-width // rel_sem.shape[0]), 8)
    rel_copies = []
    for n in range(rel_sem.shape[0]):
        lo = n * piece
        size = min(piece, width - lo)
        if size > 0:
            c = pltpu.make_async_copy(
                rel_hbm.at[pl.ds(lo, size)], rel_t.at[pl.ds(lo, size)], rel_sem.at[n])
            c.start()
            rel_copies.append(c)

    lane = lax.broadcasted_iota(jnp.int32, (rows, wide), 1)

    def put_table(step, table, tab, own):
        tab[step] = table
        for n in range(shards):
            put_packed(own.at[step, n], table[n * 16:n * 16 + 16])

    def spread(x_ref, tab, own):
        tab[0] = jnp.zeros((rows, wide), F32)
        tab[0, :, 0:width] = x_ref[...]
        x = tab[0]
        im = pltpu.roll(x, shift, axis=1)
        put_table(0, jnp.where(lane < half, x, jnp.where(lane >= hp, im, 0.0)), tab, own)

    for c in inputs[:2]:
        c.wait()
    spread(src_ref, tab_s, own_s)
    spread(dst_ref, tab_d, own_d)

    eye = lax.broadcasted_iota(jnp.int32, (rows, rows), 0) == lax.broadcasted_iota(jnp.int32, (rows, rows), 1)

    def column(x_ref):
        return jnp.sum(jnp.where(eye, jnp.broadcast_to(x_ref[...], (rows, rows)), 0.0), axis=1, keepdims=True)

    def as_row(x):
        return jnp.sum(jnp.where(eye, jnp.broadcast_to(x, (rows, rows)), 0.0), axis=0, keepdims=True)

    mine = core * chips + chip

    def gather_src(step):
        out = []
        for n, o in enumerate(others):
            c = pltpu.make_async_remote_copy(
                own_s.at[step], full_s.at[step, mine], ags_send.at[step, n], ags_recv.at[step, chip],
                device_id=(dom, peer(o) * 2 + core), device_id_type=MESH)
            c.start()
            out.append(c)
        c = pltpu.make_async_remote_copy(
            own_s.at[step], full_s.at[step, mine], fws_send.at[step, chip], fws_recv.at[step, chip],
            device_id=(dom, mate), device_id_type=MESH)
        c.start()
        out.append(c)
        full_s[step, mine] = own_s[step]
        return out

    def gather_dst(step):
        out = []
        for n, o in enumerate(offsets):
            c = pltpu.make_async_remote_copy(
                own_d.at[step], full_d.at[step, mine], agd_send.at[step, n], agd_recv.at[step, chip],
                device_id=(at_dom(step + 1), peer(o) * 2 + core), device_id_type=MESH)
            c.start()
            out.append(c)
        return out

    def forward(step, full, recv, fsend, frecv, which):
        out = []
        for o in reversed(which):
            c = peer(o)
            blk = full.at[step, core * chips + c]
            pltpu.make_async_copy(blk, blk, recv.at[step, c]).wait()
            f = pltpu.make_async_remote_copy(
                blk, blk, fsend.at[step, c], frecv.at[step, c], device_id=(dom, mate), device_id_type=MESH)
            f.start()
            out.append(f)
        return out

    def from_mate(step, full, frecv):
        for c in range(chips):
            blk = full.at[step, (1 - core) * chips + c]
            pltpu.make_async_copy(blk, blk, frecv.at[step, c]).wait()

    def place(x):
        per = rows * 2
        return lax.rem(lax.div(x, rows), 2) * hent + lax.div(x, per) * rows + lax.rem(x, rows)

    def turn_relations():
        fill = jnp.zeros((hp - half, 128), F32)
        full = nrel // 128

        def turned(ref, cols, to):
            rel_v[to, 0:hp] = jnp.concatenate([ref[0:half, cols], fill], axis=0).T
            rel_v[to, hp:wide] = jnp.concatenate([ref[half:width, cols], fill], axis=0).T

        def body(b, carry):
            cols = pl.ds(pl.multiple_of(b * 128, 128), 128)
            turned(rel_t, cols, cols)
            return carry

        lax.fori_loop(0, full, body, 0)
        if nrel % 128:
            rel_e[...] = jnp.zeros((width, 128), F32)
            rel_e[:, 0:nrel % 128] = rel_t[:, full * 128:nrel]
            turned(rel_e, slice(0, 128), slice(full * 128, full * 128 + 128))

    def prepare(step):
        tail = edges // 8 * 8
        rsp[step, tail:ep] = jnp.zeros((ep - tail, wide), F32)
        unroll = 20

        def body(b, carry):
            for u in range(unroll):
                e = b * unroll + u
                i = er_ref[step, e]
                rsp[step, pl.ds(e, 1), :] = rel_v[pl.ds(i, 1), :]
            return carry

        lax.fori_loop(0, edges // unroll, body, 0)

        def hots(ref, slot):
            ids[slot] = jnp.full((1, ep), -1, jnp.int32)
            ids[slot, :, 0:edges] = ref[step] if len(ref.shape) == 3 else ref[step:step + 1, :]
            x = ids[slot]
            return jnp.where(x < 0, -1, place(jnp.maximum(x, 0)))

        xs, xd, xn = hots(es_ref, 0), hots(ed_ref, 1), hots(ng_ref, 2)
        for m in range(0, ents, 128):
            line = lax.broadcasted_iota(jnp.int32, (128, ep), 0) + m
            s = jnp.where(line == xs, 1.0, 0.0)
            hot_t[step, m:m + 128] = s.astype(BF)
            hot[step, :, m:m + 128] = s.T.astype(BF)
            d = jnp.where(line == xd, 1.0, 0.0)
            c = jnp.sum(jnp.where(line == xn, 1.0, 0.0), axis=1, keepdims=True)
            pos[step, m:m + 128] = d
            wgt[step, m:m + 128] = d + c

    lower = pl.ds(pl.multiple_of(core * hent, hent), hent)
    upper = pl.ds(pl.multiple_of((1 - core) * hent, hent), hent)

    def split_to(full, step, side, a, b):
        for c in range(chips):
            for n in range(shards):
                blk = full.at[step, side * chips + c, n]
                at = pl.ds(pl.multiple_of(side * hent + c * rows + n * 16, 16), 16)
                a[at], b[at] = halves(unpacked(blk[0:48], tail_rows(blk, 16)))

    def rotated(step):
        for m in range(0, ep, 128):
            o = hot[step, m:m + 128]
            s = nn(o, th[...]) + nn(o, tl[...])
            sr, si = s[:, :hp], s[:, hp:]
            rr, ri = rsp[step, m:m + 128, :hp], rsp[step, m:m + 128, hp:]
            qh[m:m + 128, :hp], ql[m:m + 128, :hp] = halves(sr * rr - si * ri)
            qh[m:m + 128, hp:], ql[m:m + 128, hp:] = halves(sr * ri + si * rr)

    def weights(step, side):
        for m in range(0, hent, 128):
            at = pl.ds(pl.multiple_of(side * hent + m, 128), 128)
            a, b = dh[at], dl[at]
            s = nt(a, qh[...]) + (nt(a, ql[...]) + nt(b, qh[...]))
            w = jax.nn.sigmoid(s) * wgt[step, at] - pos[step, at]
            wth[at], wtl[at] = halves(w)

    def dst_part(which):
        a, b = wth[which], wtl[which]
        return nn(a, qh[...]) + (nn(a, ql[...]) + nn(b, qh[...]))

    def edge_grads(step):
        for m in range(0, ents, 128):
            wh[:, m:m + 128] = wth[m:m + 128].T
            wl[:, m:m + 128] = wtl[m:m + 128].T
        for m in range(0, ep, 128):
            a, b = wh[m:m + 128], wl[m:m + 128]
            g = nn(a, dh[...]) + (nn(a, dl[...]) + nn(b, dh[...]))
            gr, gi = g[:, :hp], g[:, hp:]
            rr, ri = rsp[step, m:m + 128, :hp], rsp[step, m:m + 128, hp:]
            qh[m:m + 128, :hp], ql[m:m + 128, :hp] = halves(gr * rr + gi * ri)
            qh[m:m + 128, hp:], ql[m:m + 128, hp:] = halves(gi * rr - gr * ri)

    def src_part(step, which):
        o = hot_t[step, which]
        return nn(o, qh[...]) + nn(o, ql[...])

    def to_mate(step, t, part, sib):
        c = pltpu.make_async_remote_copy(
            part.at[step], sib.at[step], dd_send.at[step, t], dd_recv.at[step, t],
            device_id=(dom, mate), device_id_type=MESH)
        c.start()
        return c

    def to_owners(step, copy, part, sib, total, red, send, recv, target, which):
        copy.wait_recv()
        for c in range(chips):
            for n in range(shards):
                at = slice(c * rows + n * 16, c * rows + n * 16 + 16)
                put_packed(total.at[step, c, n], part[at] + sib[step, at])
        out = []
        for n, o in enumerate(which):
            c = peer(o)
            r = pltpu.make_async_remote_copy(
                total.at[step, c], red.at[step, chip], send.at[step, n], recv.at[step, chip],
                device_id=(target, c * 2 + core), device_id_type=MESH)
            r.start()
            out.append(r)
        if len(which) < chips:
            red[step, chip] = total[step, chip]
        return out

    def arrived(step, red, recv, which):
        for o in reversed(which):
            blk = red.at[step, peer(o)]
            pltpu.make_async_copy(blk, blk, recv.at[step, peer(o)]).wait()
        out = []
        for n in range(shards):
            g, tails = red[step, 0, n, 0:48], tail_rows(red.at[step, 0, n], 16)
            for c in range(1, chips):
                g = g + red[step, c, n, 0:48]
                tails = [t + u for t, u in zip(tails, tail_rows(red.at[step, c, n], 16))]
            out.append(unpacked(g, tails))
        return out[0] if shards == 1 else jnp.concatenate(out, axis=0)

    def adagrad(table, state, g):
        state = state + jnp.sum(g * g, axis=1, keepdims=True) / width
        return table - LEARN_RATE * g / (jnp.sqrt(state) + EPSILON), state

    pl.semaphore_wait(bar, count)

    sent = []
    sent += gather_src(0)
    sent += gather_dst(0)
    for c in inputs[2:] + rel_copies:
        c.wait()
    src_state = column(sst_ref)
    dst_state = column(dstt_ref)
    turn_relations()
    prepare(0)

    for step in range(2):
        if step == 0:
            sent += forward(step, full_s, ags_recv, fws_send, fws_recv, others)
            sent += forward(step, full_d, agd_recv, fwd_send, fwd_recv, offsets)
            split_to(full_s, step, core, th, tl)
            from_mate(step, full_s, fws_recv)
            split_to(full_s, step, 1 - core, th, tl)
            rotated(step)
            split_to(full_d, step, core, dh, dl)
            weights(step, core)
            from_mate(step, full_d, fwd_recv)
            split_to(full_d, step, 1 - core, dh, dl)
        else:
            sent += forward(step, full_d, agd_recv, fwd_send, fwd_recv, offsets)
            split_to(full_d, step, core, dh, dl)
            from_mate(step, full_d, fwd_recv)
            split_to(full_d, step, 1 - core, dh, dl)
            sent += forward(step, full_s, ags_recv, fws_send, fws_recv, others)
            split_to(full_s, step, core, th, tl)
            from_mate(step, full_s, fws_recv)
            split_to(full_s, step, 1 - core, th, tl)
            rotated(step)
            weights(step, core)
        weights(step, 1 - core)
        part_d[step] = dst_part(upper)
        cd = to_mate(step, 0, part_d, sib_d)
        mine_d = dst_part(lower)
        sent += to_owners(step, cd, mine_d, sib_d, sum_d, red_d, rsd_send, rsd_recv, at_dom(-step - 1), offsets)
        edge_grads(step)
        part_s[step] = src_part(step, upper)
        cs = to_mate(step, 1, part_s, sib_s)
        mine_s = src_part(step, lower)
        sent += to_owners(step, cs, mine_s, sib_s, sum_s, red_s, rss_send, rss_recv, dom, others)
        if step == 0:
            prepare(1)
        g = arrived(step, red_d, rsd_recv, offsets)
        table, dst_state = adagrad(tab_d[step], dst_state, g)
        if step == 0:
            put_table(1, table, tab_d, own_d)
            sent += gather_dst(1)
        else:
            out_ref[rows:2 * rows] = table
            out_ref[2 * rows + 1:2 * rows + 2, 0:rows] = as_row(dst_state)
        g = arrived(step, red_s, rss_recv, others)
        table, src_state = adagrad(tab_s[step], src_state, g)
        if step == 0:
            put_table(1, table, tab_s, own_s)
            sent += gather_src(1)
        else:
            out_ref[0:rows] = table
            out_ref[2 * rows:2 * rows + 1, 0:rows] = as_row(src_state)
        sent += [cd, cs]
    for c in sent:
        c.wait_send()


def finish(half, res_ref, src_out, sst_out, dst_out, dstt_out):
    rows, width = src_out.shape
    wide = res_ref.shape[1]
    lane = lax.broadcasted_iota(jnp.int32, (rows, wide), 1)
    for first, out in ((0, src_out), (rows, dst_out)):
        x = res_ref[first:first + rows]
        im = pltpu.roll(x, wide // 2 + half, axis=1)
        out[...] = jnp.where(lane < half, x, im)[:, :width]
    sst_out[...] = res_ref[2 * rows:2 * rows + 1, 0:rows]
    dstt_out[...] = res_ref[2 * rows + 1:2 * rows + 2, 0:rows]


def solution(mesh):
    doms, edge_axis = mesh.shape["dom"], mesh.shape["edge"]
    chips = edge_axis // 2

    def on_device(
        src_table, src_state, dst_table, dst_state, relations, edge_src, edge_rel, edge_dst, negatives
    ):
        rows, width = src_table.shape
        half = width // 2
        wide = 2 * up(half, 128)
        ents = rows * edge_axis
        edges = edge_src.shape[1]
        ep = up(edges, 128)
        nrel = relations.shape[0]
        vm, dma = pltpu.VMEM, pltpu.SemaphoreType.DMA
        in_vmem = pl.BlockSpec(memory_space=pltpu.VMEM)
        in_hbm = pl.BlockSpec(memory_space=pltpu.HBM)
        shards = rows // 16
        block = (shards, MSG, 128)
        shard = jax.ShapeDtypeStruct((rows, width), F32)
        line = jax.ShapeDtypeStruct((1, rows), F32)
        packed = pl.pallas_call(
            functools.partial(kernel, doms, chips, half),
            out_shape=jax.ShapeDtypeStruct((2 * rows + 8, wide), F32),
            in_specs=[in_hbm] * 9,
            out_specs=in_vmem,
            scratch_shapes=[
                vm((rows, width), F32),
                vm((1, rows), F32),
                vm((rows, width), F32),
                vm((1, rows), F32),
                vm((2, edges), jnp.int32),
                pltpu.SMEM((2, edges), jnp.int32),
                vm((2, edges), jnp.int32),
                vm(negatives.shape, jnp.int32),
                vm((width, nrel), F32),
                vm((width, 128), F32),
                vm((up(nrel, 128), wide), F32),
                vm((2, ep, wide), F32),
                vm((2, ep, ents), BF),
                vm((2, ents, ep), BF),
                vm((2, ents, ep), F32),
                vm((2, ents, ep), F32),
                vm((3, 1, ep), jnp.int32),
            ]
            + [vm((2, rows, wide), F32)] * 2
            + [vm((2,) + block, F32)] * 2
            + [vm((2, edge_axis) + block, F32)] * 2
            + [vm((2, ents // 2, wide), F32)] * 4
            + [vm((2, chips) + block, F32)] * 4
            + [vm((ep, wide), BF)] * 2
            + [vm((ents, wide), BF)] * 4
            + [vm((ents, ep), BF)] * 2
            + [vm((ep, ents), BF)] * 2
            + [dma((8,))] * 2
            + [dma((2, chips))] * 8
            + [dma((2, 2))] * 2
            + [dma((2, chips))] * 4,
            compiler_params=pltpu.CompilerParams(
                collective_id=0, has_side_effects=True, vmem_limit_bytes=50 * 1024 * 1024
            ),
        )(
            *(pltpu.with_memory_space_constraint(a, pltpu.HBM) for a in (
            src_table,
            src_state.reshape(1, rows),
            dst_table,
            dst_state.reshape(1, rows),
            relations.T,
            edge_src,
            edge_rel,
            edge_dst,
            negatives,
            )),
        )
        out = pl.pallas_call(
            functools.partial(finish, half),
            out_shape=(shard, line, shard, line),
            in_specs=[in_vmem],
            out_specs=(in_vmem,) * 4,
            compiler_params=pltpu.CompilerParams(vmem_limit_bytes=1024 * 1024),
        )(packed)
        return out[0], out[1].reshape(rows), out[2], out[3].reshape(rows)

    return jax.shard_map(
        on_device,
        mesh=mesh,
        in_specs=(
            P(("dom", "edge"), None),
            P(("dom", "edge")),
            P(("dom", "edge"), None),
            P(("dom", "edge")),
            P(),
            P(None, ("dom", "edge")),
            P(None, ("dom", "edge")),
            P(None, ("dom", "edge")),
            P(None, ("dom", "edge"), None),
        ),
        out_specs=(
            P(("dom", "edge"), None),
            P(("dom", "edge")),
            P(("dom", "edge"), None),
            P(("dom", "edge")),
        ),
        check_vma=False,
    )
```

```python
import functools

import jax
import jax.numpy as jnp
from jax import lax
from jax.experimental import pallas as pl
from jax.experimental.pallas import tpu as pltpu
from jax.sharding import PartitionSpec as P

MESH = pl.DeviceIdType.MESH
LEARN_RATE = 0.1
EPSILON = 1e-06
MSG = 50
BF = jnp.bfloat16
F32 = jnp.float32


def up(n, m):
    return (n + m - 1) // m * m


def halves(x):
    hi = x.astype(BF)
    return hi, (x - hi.astype(F32)).astype(BF)


def nn(a, b):
    return jnp.dot(a, b, preferred_element_type=F32)


def nt(a, b):
    return lax.dot_general(a, b, (((1,), (1,)), ((), ())), preferred_element_type=F32)


def lanes(n):
    return lax.broadcasted_iota(jnp.int32, (n, 128), 1)


def packed_rows(x):
    a0, a1, b0, b1 = (x[:, n * 128:(n + 1) * 128] for n in range(4))
    lane = lanes(x.shape[0])
    both = jnp.where(lane < 64, a1, pltpu.roll(b1, 64, axis=1))
    left = jnp.where(lane < 8, pltpu.roll(a1, 64, axis=1), jnp.where(lane < 16, pltpu.roll(b1, 72, axis=1), 0.0))
    for n in (16, 32, 64):
        left = left + pltpu.roll(left, n, axis=1)
    line = lax.rem(lax.broadcasted_iota(jnp.int32, lane.shape, 0), 8)
    left = jnp.where(lax.div(lane, 16) == 7 - line, left, 0.0)
    tails = [jnp.sum(left[t:t + 8], axis=0, keepdims=True) for t in range(0, x.shape[0], 8)]
    return a0, b0, both, tails


def put_packed(ref, x):
    a0, b0, both, tails = packed_rows(x)
    n = x.shape[0]
    ref[0:n] = a0
    ref[n:2 * n] = b0
    ref[2 * n:3 * n] = both
    for t, row in enumerate(tails):
        ref[3 * n + t:3 * n + t + 1] = row


def unpacked(x, tails):
    n = x.shape[0] // 3
    lane = lanes(n)
    a0, b0, both = x[0:n], x[n:2 * n], x[2 * n:3 * n]
    re = []
    for row in tails:
        v = jnp.broadcast_to(pltpu.roll(row, 80, axis=1), (8, 128))
        re.append(pltpu.roll(v, 0, axis=1, stride=16, stride_axis=0))
    re = jnp.concatenate(re, axis=0)
    im = pltpu.roll(re, 120, axis=1)
    a1 = jnp.where(lane < 64, both, jnp.where(lane < 72, re, 0.0))
    b1 = jnp.where(lane < 64, pltpu.roll(both, 64, axis=1), jnp.where(lane < 72, im, 0.0))
    return jnp.concatenate([a0, a1, b0, b1], axis=1)


def tail_rows(x_ref, n):
    return [x_ref[3 * n + t:3 * n + t + 1] for t in range(n // 8)]


def kernel(
    doms, chips, half,
    src_hbm, sst_hbm, dst_hbm, dstt_hbm, rel_hbm, es_hbm, er_hbm, ed_hbm, ng_hbm,
    out_ref,
    src_ref, sst_ref, dst_ref, dstt_ref, es_ref, er_ref, ed_ref, ng_ref,
    rel_t, rel_e, rel_v, rsp, hot, hot_t, wgt, pos, ids,
    tab_s, tab_d, own_s, own_d, full_s, full_d, part_s, part_d, sib_s, sib_d, sum_s, sum_d, red_s, red_d,
    qh, ql, dh, dl, th, tl, wth, wtl, wh, wl,
    in_sem, rel_sem, ags_send, ags_recv, agd_send, agd_recv, fws_send, fws_recv, fwd_send, fwd_recv,
    dd_send, dd_recv, rss_send, rss_recv, rsd_send, rsd_recv,
):
    rows, width = src_ref.shape
    hp = up(half, 128)
    wide = 2 * hp
    ents = th.shape[0]
    hent = ents // 2
    shards = rows // 16
    edges = es_ref.shape[1]
    ep = rsp.shape[1]
    nrel = rel_hbm.shape[1]
    shift = hp - half

    dom = lax.axis_index("dom")
    k = lax.axis_index("edge")
    core = lax.rem(k, 2)
    chip = lax.div(k, 2)
    mate = chip * 2 + (1 - core)
    nx = chips // 2

    def at_dom(step):
        return lax.rem(dom + step + doms, doms)

    def far(o):
        return min(o[0], nx - o[0]) + 2 * o[1]

    offsets = sorted(((dx, dy) for dx in range(nx) for dy in range(2)), key=lambda o: -far(o))
    others = [o for o in offsets if o != (0, 0)]

    def peer(o):
        return lax.rem(lax.div(chip, 2) + o[0], nx) * 2 + lax.rem(lax.rem(chip, 2) + o[1], 2)

    bar = pltpu.get_barrier_semaphore()
    count = 1
    for other in (at_dom(1), at_dom(-1)):
        for o in offsets:
            pl.semaphore_signal(bar, inc=1, device_id=(other, peer(o) * 2 + core), device_id_type=MESH)
            count += 1
    for o in others:
        pl.semaphore_signal(bar, inc=1, device_id=(dom, peer(o) * 2 + core), device_id_type=MESH)
        count += 1
    pl.semaphore_signal(bar, inc=1, device_id=(dom, mate), device_id_type=MESH)

    inputs = []
    for n, (a, b) in enumerate((
        (src_hbm, src_ref), (dst_hbm, dst_ref), (sst_hbm, sst_ref), (dstt_hbm, dstt_ref),
        (es_hbm, es_ref), (er_hbm, er_ref), (ed_hbm, ed_ref), (ng_hbm, ng_ref),
    )):
        c = pltpu.make_async_copy(a, b, in_sem.at[n])
        c.start()
        inputs.append(c)
    piece = up(-(-width // rel_sem.shape[0]), 8)
    rel_copies = []
    for n in range(rel_sem.shape[0]):
        lo = n * piece
        size = min(piece, width - lo)
        if size > 0:
            c = pltpu.make_async_copy(
                rel_hbm.at[pl.ds(lo, size)], rel_t.at[pl.ds(lo, size)], rel_sem.at[n])
            c.start()
            rel_copies.append(c)

    lane = lax.broadcasted_iota(jnp.int32, (rows, wide), 1)

    def put_table(step, table, tab, own):
        tab[step] = table
        for n in range(shards):
            put_packed(own.at[step, n], table[n * 16:n * 16 + 16])

    def spread(x_ref, tab, own):
        tab[0] = jnp.zeros((rows, wide), F32)
        tab[0, :, 0:width] = x_ref[...]
        x = tab[0]
        im = pltpu.roll(x, shift, axis=1)
        put_table(0, jnp.where(lane < half, x, jnp.where(lane >= hp, im, 0.0)), tab, own)

    for c in inputs[:2]:
        c.wait()
    spread(src_ref, tab_s, own_s)
    spread(dst_ref, tab_d, own_d)

    eye = lax.broadcasted_iota(jnp.int32, (rows, rows), 0) == lax.broadcasted_iota(jnp.int32, (rows, rows), 1)

    def column(x_ref):
        return jnp.sum(jnp.where(eye, jnp.broadcast_to(x_ref[...], (rows, rows)), 0.0), axis=1, keepdims=True)

    def as_row(x):
        return jnp.sum(jnp.where(eye, jnp.broadcast_to(x, (rows, rows)), 0.0), axis=0, keepdims=True)

    mine = core * chips + chip

    def gather_src(step):
        out = []
        for n, o in enumerate(others):
            c = pltpu.make_async_remote_copy(
                own_s.at[step], full_s.at[step, mine], ags_send.at[step, n], ags_recv.at[step, chip],
                device_id=(dom, peer(o) * 2 + core), device_id_type=MESH)
            c.start()
            out.append(c)
        c = pltpu.make_async_remote_copy(
            own_s.at[step], full_s.at[step, mine], fws_send.at[step, chip], fws_recv.at[step, chip],
            device_id=(dom, mate), device_id_type=MESH)
        c.start()
        out.append(c)
        full_s[step, mine] = own_s[step]
        return out

    def gather_dst(step):
        out = []
        for n, o in enumerate(offsets):
            c = pltpu.make_async_remote_copy(
                own_d.at[step], full_d.at[step, mine], agd_send.at[step, n], agd_recv.at[step, chip],
                device_id=(at_dom(step + 1), peer(o) * 2 + core), device_id_type=MESH)
            c.start()
            out.append(c)
        return out

    def forward(step, full, recv, fsend, frecv, which):
        out = []
        for o in reversed(which):
            c = peer(o)
            blk = full.at[step, core * chips + c]
            pltpu.make_async_copy(blk, blk, recv.at[step, c]).wait()
            f = pltpu.make_async_remote_copy(
                blk, blk, fsend.at[step, c], frecv.at[step, c], device_id=(dom, mate), device_id_type=MESH)
            f.start()
            out.append(f)
        return out

    def from_mate(step, full, frecv):
        for c in range(chips):
            blk = full.at[step, (1 - core) * chips + c]
            pltpu.make_async_copy(blk, blk, frecv.at[step, c]).wait()

    def place(x):
        per = rows * 2
        return lax.rem(lax.div(x, rows), 2) * hent + lax.div(x, per) * rows + lax.rem(x, rows)

    def turn_relations():
        fill = jnp.zeros((hp - half, 128), F32)
        full = nrel // 128

        def turned(ref, cols, to):
            rel_v[to, 0:hp] = jnp.concatenate([ref[0:half, cols], fill], axis=0).T
            rel_v[to, hp:wide] = jnp.concatenate([ref[half:width, cols], fill], axis=0).T

        def body(b, carry):
            cols = pl.ds(pl.multiple_of(b * 128, 128), 128)
            turned(rel_t, cols, cols)
            return carry

        lax.fori_loop(0, full, body, 0)
        if nrel % 128:
            rel_e[...] = jnp.zeros((width, 128), F32)
            rel_e[:, 0:nrel % 128] = rel_t[:, full * 128:nrel]
            turned(rel_e, slice(0, 128), slice(full * 128, full * 128 + 128))

    def prepare(step):
        tail = edges // 8 * 8
        rsp[step, tail:ep] = jnp.zeros((ep - tail, wide), F32)
        unroll = 20

        def body(b, carry):
            for u in range(unroll):
                e = b * unroll + u
                i = er_ref[step, e]
                rsp[step, pl.ds(e, 1), :] = rel_v[pl.ds(i, 1), :]
            return carry

        lax.fori_loop(0, edges // unroll, body, 0)

        def hots(ref, slot):
            ids[slot] = jnp.full((1, ep), -1, jnp.int32)
            ids[slot, :, 0:edges] = ref[step] if len(ref.shape) == 3 else ref[step:step + 1, :]
            x = ids[slot]
            return jnp.where(x < 0, -1, place(jnp.maximum(x, 0)))

        xs, xd, xn = hots(es_ref, 0), hots(ed_ref, 1), hots(ng_ref, 2)
        for m in range(0, ents, 128):
            line = lax.broadcasted_iota(jnp.int32, (128, ep), 0) + m
            s = jnp.where(line == xs, 1.0, 0.0)
            hot_t[step, m:m + 128] = s.astype(BF)
            hot[step, :, m:m + 128] = s.T.astype(BF)
            d = jnp.where(line == xd, 1.0, 0.0)
            c = jnp.sum(jnp.where(line == xn, 1.0, 0.0), axis=1, keepdims=True)
            pos[step, m:m + 128] = d
            wgt[step, m:m + 128] = d + c

    lower = pl.ds(pl.multiple_of(core * hent, hent), hent)
    upper = pl.ds(pl.multiple_of((1 - core) * hent, hent), hent)

    def split_to(full, step, side, a, b):
        for c in range(chips):
            for n in range(shards):
                blk = full.at[step, side * chips + c, n]
                at = pl.ds(pl.multiple_of(side * hent + c * rows + n * 16, 16), 16)
                a[at], b[at] = halves(unpacked(blk[0:48], tail_rows(blk, 16)))

    def rotated(step):
        for m in range(0, ep, 128):
            o = hot[step, m:m + 128]
            s = nn(o, th[...]) + nn(o, tl[...])
            sr, si = s[:, :hp], s[:, hp:]
            rr, ri = rsp[step, m:m + 128, :hp], rsp[step, m:m + 128, hp:]
            qh[m:m + 128, :hp], ql[m:m + 128, :hp] = halves(sr * rr - si * ri)
            qh[m:m + 128, hp:], ql[m:m + 128, hp:] = halves(sr * ri + si * rr)

    def weights(step, side):
        for m in range(0, hent, 128):
            at = pl.ds(pl.multiple_of(side * hent + m, 128), 128)
            a, b = dh[at], dl[at]
            s = nt(a, qh[...]) + (nt(a, ql[...]) + nt(b, qh[...]))
            w = jax.nn.sigmoid(s) * wgt[step, at] - pos[step, at]
            wth[at], wtl[at] = halves(w)

    def dst_part(which):
        a, b = wth[which], wtl[which]
        return nn(a, qh[...]) + (nn(a, ql[...]) + nn(b, qh[...]))

    def edge_grads(step):
        for m in range(0, ents, 128):
            wh[:, m:m + 128] = wth[m:m + 128].T
            wl[:, m:m + 128] = wtl[m:m + 128].T
        for m in range(0, ep, 128):
            a, b = wh[m:m + 128], wl[m:m + 128]
            g = nn(a, dh[...]) + (nn(a, dl[...]) + nn(b, dh[...]))
            gr, gi = g[:, :hp], g[:, hp:]
            rr, ri = rsp[step, m:m + 128, :hp], rsp[step, m:m + 128, hp:]
            qh[m:m + 128, :hp], ql[m:m + 128, :hp] = halves(gr * rr + gi * ri)
            qh[m:m + 128, hp:], ql[m:m + 128, hp:] = halves(gi * rr - gr * ri)

    def src_part(step, which):
        o = hot_t[step, which]
        return nn(o, qh[...]) + nn(o, ql[...])

    def to_mate(step, t, part, sib):
        c = pltpu.make_async_remote_copy(
            part.at[step], sib.at[step], dd_send.at[step, t], dd_recv.at[step, t],
            device_id=(dom, mate), device_id_type=MESH)
        c.start()
        return c

    def to_owners(step, copy, part, sib, total, red, send, recv, target, which):
        copy.wait_recv()
        for c in range(chips):
            for n in range(shards):
                at = slice(c * rows + n * 16, c * rows + n * 16 + 16)
                put_packed(total.at[step, c, n], part[at] + sib[step, at])
        out = []
        for n, o in enumerate(which):
            c = peer(o)
            r = pltpu.make_async_remote_copy(
                total.at[step, c], red.at[step, chip], send.at[step, n], recv.at[step, chip],
                device_id=(target, c * 2 + core), device_id_type=MESH)
            r.start()
            out.append(r)
        if len(which) < chips:
            red[step, chip] = total[step, chip]
        return out

    def arrived(step, red, recv, which):
        for o in reversed(which):
            blk = red.at[step, peer(o)]
            pltpu.make_async_copy(blk, blk, recv.at[step, peer(o)]).wait()
        out = []
        for n in range(shards):
            g, tails = red[step, 0, n, 0:48], tail_rows(red.at[step, 0, n], 16)
            for c in range(1, chips):
                g = g + red[step, c, n, 0:48]
                tails = [t + u for t, u in zip(tails, tail_rows(red.at[step, c, n], 16))]
            out.append(unpacked(g, tails))
        return out[0] if shards == 1 else jnp.concatenate(out, axis=0)

    def adagrad(table, state, g):
        state = state + jnp.sum(g * g, axis=1, keepdims=True) / width
        return table - LEARN_RATE * g / (jnp.sqrt(state) + EPSILON), state

    pl.semaphore_wait(bar, count)

    sent = []
    sent += gather_src(0)
    sent += gather_dst(0)
    for c in inputs[2:] + rel_copies:
        c.wait()
    src_state = column(sst_ref)
    dst_state = column(dstt_ref)
    turn_relations()
    prepare(0)

    for step in range(2):
        if step == 0:
            sent += forward(step, full_s, ags_recv, fws_send, fws_recv, others)
            sent += forward(step, full_d, agd_recv, fwd_send, fwd_recv, offsets)
            split_to(full_s, step, core, th, tl)
            from_mate(step, full_s, fws_recv)
            split_to(full_s, step, 1 - core, th, tl)
            rotated(step)
            split_to(full_d, step, core, dh, dl)
            weights(step, core)
            from_mate(step, full_d, fwd_recv)
            split_to(full_d, step, 1 - core, dh, dl)
        else:
            sent += forward(step, full_d, agd_recv, fwd_send, fwd_recv, offsets)
            split_to(full_d, step, core, dh, dl)
            from_mate(step, full_d, fwd_recv)
            split_to(full_d, step, 1 - core, dh, dl)
            sent += forward(step, full_s, ags_recv, fws_send, fws_recv, others)
            split_to(full_s, step, core, th, tl)
            from_mate(step, full_s, fws_recv)
            split_to(full_s, step, 1 - core, th, tl)
            rotated(step)
        weights(step, 1 - core)
        part_d[step] = dst_part(upper)
        cd = to_mate(step, 0, part_d, sib_d)
        if step == 1:
            weights(step, core)
        mine_d = dst_part(lower)
        edge_grads(step)
        part_s[step] = src_part(step, upper)
        cs = to_mate(step, 1, part_s, sib_s)
        sent += to_owners(step, cd, mine_d, sib_d, sum_d, red_d, rsd_send, rsd_recv, at_dom(-step - 1), offsets)
        mine_s = src_part(step, lower)
        sent += to_owners(step, cs, mine_s, sib_s, sum_s, red_s, rss_send, rss_recv, dom, others)
        if step == 0:
            prepare(1)
        g = arrived(step, red_d, rsd_recv, offsets)
        table, dst_state = adagrad(tab_d[step], dst_state, g)
        if step == 0:
            put_table(1, table, tab_d, own_d)
            sent += gather_dst(1)
        else:
            out_ref[rows:2 * rows] = table
            out_ref[2 * rows + 1:2 * rows + 2, 0:rows] = as_row(dst_state)
        g = arrived(step, red_s, rss_recv, others)
        table, src_state = adagrad(tab_s[step], src_state, g)
        if step == 0:
            put_table(1, table, tab_s, own_s)
            sent += gather_src(1)
        else:
            out_ref[0:rows] = table
            out_ref[2 * rows:2 * rows + 1, 0:rows] = as_row(src_state)
        sent += [cd, cs]
    for c in sent:
        c.wait_send()


def finish(half, res_ref, src_out, sst_out, dst_out, dstt_out):
    rows, width = src_out.shape
    wide = res_ref.shape[1]
    lane = lax.broadcasted_iota(jnp.int32, (rows, wide), 1)
    for first, out in ((0, src_out), (rows, dst_out)):
        x = res_ref[first:first + rows]
        im = pltpu.roll(x, wide // 2 + half, axis=1)
        out[...] = jnp.where(lane < half, x, im)[:, :width]
    sst_out[...] = res_ref[2 * rows:2 * rows + 1, 0:rows]
    dstt_out[...] = res_ref[2 * rows + 1:2 * rows + 2, 0:rows]


def solution(mesh):
    doms, edge_axis = mesh.shape["dom"], mesh.shape["edge"]
    chips = edge_axis // 2

    def on_device(
        src_table, src_state, dst_table, dst_state, relations, edge_src, edge_rel, edge_dst, negatives
    ):
        rows, width = src_table.shape
        half = width // 2
        wide = 2 * up(half, 128)
        ents = rows * edge_axis
        edges = edge_src.shape[1]
        ep = up(edges, 128)
        nrel = relations.shape[0]
        vm, dma = pltpu.VMEM, pltpu.SemaphoreType.DMA
        in_vmem = pl.BlockSpec(memory_space=pltpu.VMEM)
        in_hbm = pl.BlockSpec(memory_space=pltpu.HBM)
        shards = rows // 16
        block = (shards, MSG, 128)
        shard = jax.ShapeDtypeStruct((rows, width), F32)
        line = jax.ShapeDtypeStruct((1, rows), F32)
        packed = pl.pallas_call(
            functools.partial(kernel, doms, chips, half),
            out_shape=jax.ShapeDtypeStruct((2 * rows + 8, wide), F32),
            in_specs=[in_hbm] * 9,
            out_specs=in_vmem,
            scratch_shapes=[
                vm((rows, width), F32),
                vm((1, rows), F32),
                vm((rows, width), F32),
                vm((1, rows), F32),
                vm((2, edges), jnp.int32),
                pltpu.SMEM((2, edges), jnp.int32),
                vm((2, edges), jnp.int32),
                vm(negatives.shape, jnp.int32),
                vm((width, nrel), F32),
                vm((width, 128), F32),
                vm((up(nrel, 128), wide), F32),
                vm((2, ep, wide), F32),
                vm((2, ep, ents), BF),
                vm((2, ents, ep), BF),
                vm((2, ents, ep), F32),
                vm((2, ents, ep), F32),
                vm((3, 1, ep), jnp.int32),
            ]
            + [vm((2, rows, wide), F32)] * 2
            + [vm((2,) + block, F32)] * 2
            + [vm((2, edge_axis) + block, F32)] * 2
            + [vm((2, ents // 2, wide), F32)] * 4
            + [vm((2, chips) + block, F32)] * 4
            + [vm((ep, wide), BF)] * 2
            + [vm((ents, wide), BF)] * 4
            + [vm((ents, ep), BF)] * 2
            + [vm((ep, ents), BF)] * 2
            + [dma((8,))] * 2
            + [dma((2, chips))] * 8
            + [dma((2, 2))] * 2
            + [dma((2, chips))] * 4,
            compiler_params=pltpu.CompilerParams(
                collective_id=0, has_side_effects=True, vmem_limit_bytes=50 * 1024 * 1024
            ),
        )(
            *(pltpu.with_memory_space_constraint(a, pltpu.HBM) for a in (
            src_table,
            src_state.reshape(1, rows),
            dst_table,
            dst_state.reshape(1, rows),
            relations.T,
            edge_src,
            edge_rel,
            edge_dst,
            negatives,
            )),
        )
        out = pl.pallas_call(
            functools.partial(finish, half),
            out_shape=(shard, line, shard, line),
            in_specs=[in_vmem],
            out_specs=(in_vmem,) * 4,
            compiler_params=pltpu.CompilerParams(vmem_limit_bytes=1024 * 1024),
        )(packed)
        return out[0], out[1].reshape(rows), out[2], out[3].reshape(rows)

    return jax.shard_map(
        on_device,
        mesh=mesh,
        in_specs=(
            P(("dom", "edge"), None),
            P(("dom", "edge")),
            P(("dom", "edge"), None),
            P(("dom", "edge")),
            P(),
            P(None, ("dom", "edge")),
            P(None, ("dom", "edge")),
            P(None, ("dom", "edge")),
            P(None, ("dom", "edge"), None),
        ),
        out_specs=(
            P(("dom", "edge"), None),
            P(("dom", "edge")),
            P(("dom", "edge"), None),
            P(("dom", "edge")),
        ),
        check_vma=False,
    )
```

```python
import functools

import jax
import jax.numpy as jnp
from jax import lax
from jax.experimental import pallas as pl
from jax.experimental.pallas import tpu as pltpu
from jax.sharding import PartitionSpec as P

MESH = pl.DeviceIdType.MESH
LEARN_RATE = 0.1
EPSILON = 1e-06
MSG = 50
BF = jnp.bfloat16
F32 = jnp.float32


def up(n, m):
    return (n + m - 1) // m * m


def halves(x):
    hi = x.astype(BF)
    return hi, (x - hi.astype(F32)).astype(BF)


def nn(a, b):
    return jnp.dot(a, b, preferred_element_type=F32)


def nt(a, b):
    return lax.dot_general(a, b, (((1,), (1,)), ((), ())), preferred_element_type=F32)


def lanes(n):
    return lax.broadcasted_iota(jnp.int32, (n, 128), 1)


def packed_rows(x):
    a0, a1, b0, b1 = (x[:, n * 128:(n + 1) * 128] for n in range(4))
    lane = lanes(x.shape[0])
    both = jnp.where(lane < 64, a1, pltpu.roll(b1, 64, axis=1))
    left = jnp.where(lane < 8, pltpu.roll(a1, 64, axis=1), jnp.where(lane < 16, pltpu.roll(b1, 72, axis=1), 0.0))
    for n in (16, 32, 64):
        left = left + pltpu.roll(left, n, axis=1)
    line = lax.rem(lax.broadcasted_iota(jnp.int32, lane.shape, 0), 8)
    left = jnp.where(lax.div(lane, 16) == 7 - line, left, 0.0)
    tails = [jnp.sum(left[t:t + 8], axis=0, keepdims=True) for t in range(0, x.shape[0], 8)]
    return a0, b0, both, tails


def put_packed(ref, x):
    a0, b0, both, tails = packed_rows(x)
    n = x.shape[0]
    ref[0:n] = a0
    ref[n:2 * n] = b0
    ref[2 * n:3 * n] = both
    for t, row in enumerate(tails):
        ref[3 * n + t:3 * n + t + 1] = row


def unpacked(x, tails):
    n = x.shape[0] // 3
    lane = lanes(n)
    a0, b0, both = x[0:n], x[n:2 * n], x[2 * n:3 * n]
    re = []
    for row in tails:
        v = jnp.broadcast_to(pltpu.roll(row, 80, axis=1), (8, 128))
        re.append(pltpu.roll(v, 0, axis=1, stride=16, stride_axis=0))
    re = jnp.concatenate(re, axis=0)
    im = pltpu.roll(re, 120, axis=1)
    a1 = jnp.where(lane < 64, both, jnp.where(lane < 72, re, 0.0))
    b1 = jnp.where(lane < 64, pltpu.roll(both, 64, axis=1), jnp.where(lane < 72, im, 0.0))
    return jnp.concatenate([a0, a1, b0, b1], axis=1)


def tail_rows(x_ref, n):
    return [x_ref[3 * n + t:3 * n + t + 1] for t in range(n // 8)]


def kernel(
    doms, chips, half,
    src_hbm, sst_hbm, dst_hbm, dstt_hbm, rel_hbm, es_hbm, er_hbm, ed_hbm, ng_hbm,
    out_ref,
    src_ref, sst_ref, dst_ref, dstt_ref, es_ref, er_ref, ed_ref, ng_ref,
    rel_t, rel_e, rel_v, rsp, hot, hot_t, wgt, pos, ids,
    tab_s, tab_d, own_s, own_d, full_s, full_d, part_s, part_d, sib_s, sib_d, sum_s, sum_d, red_s, red_d,
    qh, ql, dh, dl, th, tl, wth, wtl, wh, wl,
    in_sem, rel_sem, ags_send, ags_recv, agd_send, agd_recv, fws_send, fws_recv, fwd_send, fwd_recv,
    dd_send, dd_recv, rss_send, rss_recv, rsd_send, rsd_recv,
):
    rows, width = src_ref.shape
    hp = up(half, 128)
    wide = 2 * hp
    ents = th.shape[0]
    hent = ents // 2
    shards = rows // 16
    edges = es_ref.shape[1]
    ep = rsp.shape[1]
    nrel = rel_hbm.shape[1]
    shift = hp - half

    dom = lax.axis_index("dom")
    k = lax.axis_index("edge")
    core = lax.rem(k, 2)
    chip = lax.div(k, 2)
    mate = chip * 2 + (1 - core)
    nx = chips // 2

    def at_dom(step):
        return lax.rem(dom + step + doms, doms)

    def far(o):
        return min(o[0], nx - o[0]) + 2 * o[1]

    offsets = sorted(((dx, dy) for dx in range(nx) for dy in range(2)), key=lambda o: -far(o))
    others = [o for o in offsets if o != (0, 0)]

    def peer(o):
        return lax.rem(lax.div(chip, 2) + o[0], nx) * 2 + lax.rem(lax.rem(chip, 2) + o[1], 2)

    bar = pltpu.get_barrier_semaphore()
    count = 1
    for other in (at_dom(1), at_dom(-1)):
        for o in offsets:
            pl.semaphore_signal(bar, inc=1, device_id=(other, peer(o) * 2 + core), device_id_type=MESH)
            count += 1
    for o in others:
        pl.semaphore_signal(bar, inc=1, device_id=(dom, peer(o) * 2 + core), device_id_type=MESH)
        count += 1
    pl.semaphore_signal(bar, inc=1, device_id=(dom, mate), device_id_type=MESH)

    inputs = []
    for n, (a, b) in enumerate((
        (src_hbm, src_ref), (dst_hbm, dst_ref), (sst_hbm, sst_ref), (dstt_hbm, dstt_ref),
        (es_hbm, es_ref), (er_hbm, er_ref), (ed_hbm, ed_ref), (ng_hbm, ng_ref),
    )):
        c = pltpu.make_async_copy(a, b, in_sem.at[n])
        c.start()
        inputs.append(c)
    piece = up(-(-width // rel_sem.shape[0]), 8)
    rel_copies = []
    for n in range(rel_sem.shape[0]):
        lo = n * piece
        size = min(piece, width - lo)
        if size > 0:
            c = pltpu.make_async_copy(
                rel_hbm.at[pl.ds(lo, size)], rel_t.at[pl.ds(lo, size)], rel_sem.at[n])
            c.start()
            rel_copies.append(c)

    lane = lax.broadcasted_iota(jnp.int32, (rows, wide), 1)

    def put_table(step, table, tab, own):
        tab[step] = table
        for n in range(shards):
            put_packed(own.at[step, n], table[n * 16:n * 16 + 16])

    def spread(x_ref, tab, own):
        tab[0] = jnp.zeros((rows, wide), F32)
        tab[0, :, 0:width] = x_ref[...]
        x = tab[0]
        im = pltpu.roll(x, shift, axis=1)
        put_table(0, jnp.where(lane < half, x, jnp.where(lane >= hp, im, 0.0)), tab, own)

    for c in inputs[:2]:
        c.wait()
    spread(src_ref, tab_s, own_s)
    spread(dst_ref, tab_d, own_d)

    eye = lax.broadcasted_iota(jnp.int32, (rows, rows), 0) == lax.broadcasted_iota(jnp.int32, (rows, rows), 1)

    def column(x_ref):
        return jnp.sum(jnp.where(eye, jnp.broadcast_to(x_ref[...], (rows, rows)), 0.0), axis=1, keepdims=True)

    def as_row(x):
        return jnp.sum(jnp.where(eye, jnp.broadcast_to(x, (rows, rows)), 0.0), axis=0, keepdims=True)

    mine = core * chips + chip

    def gather_src(step):
        out = []
        for n, o in enumerate(others):
            c = pltpu.make_async_remote_copy(
                own_s.at[step], full_s.at[step, mine], ags_send.at[step, n], ags_recv.at[step, chip],
                device_id=(dom, peer(o) * 2 + core), device_id_type=MESH)
            c.start()
            out.append(c)
        c = pltpu.make_async_remote_copy(
            own_s.at[step], full_s.at[step, mine], fws_send.at[step, chip], fws_recv.at[step, chip],
            device_id=(dom, mate), device_id_type=MESH)
        c.start()
        out.append(c)
        full_s[step, mine] = own_s[step]
        return out

    def gather_dst(step):
        out = []
        for n, o in enumerate(offsets):
            c = pltpu.make_async_remote_copy(
                own_d.at[step], full_d.at[step, mine], agd_send.at[step, n], agd_recv.at[step, chip],
                device_id=(at_dom(step + 1), peer(o) * 2 + core), device_id_type=MESH)
            c.start()
            out.append(c)
        return out

    def forward(step, full, recv, fsend, frecv, which):
        out = []
        for o in reversed(which):
            c = peer(o)
            blk = full.at[step, core * chips + c]
            pltpu.make_async_copy(blk, blk, recv.at[step, c]).wait()
            f = pltpu.make_async_remote_copy(
                blk, blk, fsend.at[step, c], frecv.at[step, c], device_id=(dom, mate), device_id_type=MESH)
            f.start()
            out.append(f)
        return out

    def from_mate(step, full, frecv):
        for c in range(chips):
            blk = full.at[step, (1 - core) * chips + c]
            pltpu.make_async_copy(blk, blk, frecv.at[step, c]).wait()

    def place(x):
        per = rows * 2
        return lax.rem(lax.div(x, rows), 2) * hent + lax.div(x, per) * rows + lax.rem(x, rows)

    def turn_relations():
        fill = jnp.zeros((hp - half, 128), F32)
        full = nrel // 128

        def turned(ref, cols, to):
            rel_v[to, 0:hp] = jnp.concatenate([ref[0:half, cols], fill], axis=0).T
            rel_v[to, hp:wide] = jnp.concatenate([ref[half:width, cols], fill], axis=0).T

        def body(b, carry):
            cols = pl.ds(pl.multiple_of(b * 128, 128), 128)
            turned(rel_t, cols, cols)
            return carry

        lax.fori_loop(0, full, body, 0)
        if nrel % 128:
            rel_e[...] = jnp.zeros((width, 128), F32)
            rel_e[:, 0:nrel % 128] = rel_t[:, full * 128:nrel]
            turned(rel_e, slice(0, 128), slice(full * 128, full * 128 + 128))

    def prepare(step):
        tail = edges // 8 * 8
        rsp[step, tail:ep] = jnp.zeros((ep - tail, wide), F32)
        unroll = 20

        def body(b, carry):
            for u in range(unroll):
                e = b * unroll + u
                i = er_ref[step, e]
                rsp[step, pl.ds(e, 1), :] = rel_v[pl.ds(i, 1), :]
            return carry

        lax.fori_loop(0, edges // unroll, body, 0)

        def hots(ref, slot):
            ids[slot] = jnp.full((1, ep), -1, jnp.int32)
            ids[slot, :, 0:edges] = ref[step] if len(ref.shape) == 3 else ref[step:step + 1, :]
            x = ids[slot]
            return jnp.where(x < 0, -1, place(jnp.maximum(x, 0)))

        xs, xd, xn = hots(es_ref, 0), hots(ed_ref, 1), hots(ng_ref, 2)
        for m in range(0, ents, 128):
            line = lax.broadcasted_iota(jnp.int32, (128, ep), 0) + m
            s = jnp.where(line == xs, 1.0, 0.0)
            hot_t[step, m:m + 128] = s.astype(BF)
            hot[step, :, m:m + 128] = s.T.astype(BF)
            d = jnp.where(line == xd, 1.0, 0.0)
            c = jnp.sum(jnp.where(line == xn, 1.0, 0.0), axis=1, keepdims=True)
            pos[step, m:m + 128] = d
            wgt[step, m:m + 128] = d + c

    lower = pl.ds(pl.multiple_of(core * hent, hent), hent)
    upper = pl.ds(pl.multiple_of((1 - core) * hent, hent), hent)

    def split_to(full, step, side, a, b):
        for c in range(chips):
            for n in range(shards):
                blk = full.at[step, side * chips + c, n]
                at = pl.ds(pl.multiple_of(side * hent + c * rows + n * 16, 16), 16)
                a[at], b[at] = halves(unpacked(blk[0:48], tail_rows(blk, 16)))

    def rotated(step):
        for m in range(0, ep, 128):
            o = hot[step, m:m + 128]
            s = nn(o, th[...]) + nn(o, tl[...])
            sr, si = s[:, :hp], s[:, hp:]
            rr, ri = rsp[step, m:m + 128, :hp], rsp[step, m:m + 128, hp:]
            qh[m:m + 128, :hp], ql[m:m + 128, :hp] = halves(sr * rr - si * ri)
            qh[m:m + 128, hp:], ql[m:m + 128, hp:] = halves(sr * ri + si * rr)

    def weights(step, side):
        for m in range(0, hent, 128):
            at = pl.ds(pl.multiple_of(side * hent + m, 128), 128)
            a, b = dh[at], dl[at]
            s = nt(a, qh[...]) + (nt(a, ql[...]) + nt(b, qh[...]))
            w = (0.5 * jnp.tanh(0.5 * s) + 0.5) * wgt[step, at] - pos[step, at]
            wth[at], wtl[at] = halves(w)

    def dst_part(which):
        a, b = wth[which], wtl[which]
        return nn(a, qh[...]) + (nn(a, ql[...]) + nn(b, qh[...]))

    def edge_grads(step):
        for m in range(0, ents, 128):
            wh[:, m:m + 128] = wth[m:m + 128].T
            wl[:, m:m + 128] = wtl[m:m + 128].T
        for m in range(0, ep, 128):
            a, b = wh[m:m + 128], wl[m:m + 128]
            g = nn(a, dh[...]) + (nn(a, dl[...]) + nn(b, dh[...]))
            gr, gi = g[:, :hp], g[:, hp:]
            rr, ri = rsp[step, m:m + 128, :hp], rsp[step, m:m + 128, hp:]
            qh[m:m + 128, :hp], ql[m:m + 128, :hp] = halves(gr * rr + gi * ri)
            qh[m:m + 128, hp:], ql[m:m + 128, hp:] = halves(gi * rr - gr * ri)

    def src_part(step, which):
        o = hot_t[step, which]
        return nn(o, qh[...]) + nn(o, ql[...])

    def to_mate(step, t, part, sib):
        c = pltpu.make_async_remote_copy(
            part.at[step], sib.at[step], dd_send.at[step, t], dd_recv.at[step, t],
            device_id=(dom, mate), device_id_type=MESH)
        c.start()
        return c

    def to_owners(step, copy, part, sib, total, red, send, recv, target, which):
        copy.wait_recv()
        for c in range(chips):
            for n in range(shards):
                at = slice(c * rows + n * 16, c * rows + n * 16 + 16)
                put_packed(total.at[step, c, n], part[at] + sib[step, at])
        out = []
        for n, o in enumerate(which):
            c = peer(o)
            r = pltpu.make_async_remote_copy(
                total.at[step, c], red.at[step, chip], send.at[step, n], recv.at[step, chip],
                device_id=(target, c * 2 + core), device_id_type=MESH)
            r.start()
            out.append(r)
        if len(which) < chips:
            red[step, chip] = total[step, chip]
        return out

    def arrived(step, red, recv, which):
        for o in reversed(which):
            blk = red.at[step, peer(o)]
            pltpu.make_async_copy(blk, blk, recv.at[step, peer(o)]).wait()
        out = []
        for n in range(shards):
            g, tails = red[step, 0, n, 0:48], tail_rows(red.at[step, 0, n], 16)
            for c in range(1, chips):
                g = g + red[step, c, n, 0:48]
                tails = [t + u for t, u in zip(tails, tail_rows(red.at[step, c, n], 16))]
            out.append(unpacked(g, tails))
        return out[0] if shards == 1 else jnp.concatenate(out, axis=0)

    def adagrad(table, state, g):
        state = state + jnp.sum(g * g, axis=1, keepdims=True) / width
        return table - LEARN_RATE * g / (jnp.sqrt(state) + EPSILON), state

    pl.semaphore_wait(bar, count)

    sent = []
    sent += gather_dst(0)
    sent += gather_src(0)
    for c in inputs[2:] + rel_copies:
        c.wait()
    src_state = column(sst_ref)
    dst_state = column(dstt_ref)
    turn_relations()
    prepare(0)

    for step in range(2):
        if step == 0:
            sent += forward(step, full_s, ags_recv, fws_send, fws_recv, others)
            sent += forward(step, full_d, agd_recv, fwd_send, fwd_recv, offsets)
            split_to(full_s, step, core, th, tl)
            from_mate(step, full_s, fws_recv)
            split_to(full_s, step, 1 - core, th, tl)
            rotated(step)
            split_to(full_d, step, core, dh, dl)
            weights(step, core)
            from_mate(step, full_d, fwd_recv)
            split_to(full_d, step, 1 - core, dh, dl)
        else:
            sent += forward(step, full_d, agd_recv, fwd_send, fwd_recv, offsets)
            sent += forward(step, full_s, ags_recv, fws_send, fws_recv, others)
            split_to(full_s, step, core, th, tl)
            split_to(full_d, step, core, dh, dl)
            from_mate(step, full_d, fwd_recv)
            split_to(full_d, step, 1 - core, dh, dl)
            from_mate(step, full_s, fws_recv)
            split_to(full_s, step, 1 - core, th, tl)
            rotated(step)
        weights(step, 1 - core)
        part_d[step] = dst_part(upper)
        cd = to_mate(step, 0, part_d, sib_d)
        if step == 1:
            weights(step, core)
        mine_d = dst_part(lower)
        edge_grads(step)
        part_s[step] = src_part(step, upper)
        cs = to_mate(step, 1, part_s, sib_s)
        sent += to_owners(step, cd, mine_d, sib_d, sum_d, red_d, rsd_send, rsd_recv, at_dom(-step - 1), offsets)
        mine_s = src_part(step, lower)
        sent += to_owners(step, cs, mine_s, sib_s, sum_s, red_s, rss_send, rss_recv, dom, others)
        if step == 0:
            prepare(1)
        g = arrived(step, red_d, rsd_recv, offsets)
        table, dst_state = adagrad(tab_d[step], dst_state, g)
        if step == 0:
            put_table(1, table, tab_d, own_d)
            sent += gather_dst(1)
        else:
            out_ref[rows:2 * rows] = table
            out_ref[2 * rows + 1:2 * rows + 2, 0:rows] = as_row(dst_state)
        g = arrived(step, red_s, rss_recv, others)
        table, src_state = adagrad(tab_s[step], src_state, g)
        if step == 0:
            put_table(1, table, tab_s, own_s)
            sent += gather_src(1)
        else:
            out_ref[0:rows] = table
            out_ref[2 * rows:2 * rows + 1, 0:rows] = as_row(src_state)
        sent += [cd, cs]
    for c in sent:
        c.wait_send()


def finish(half, res_ref, src_out, sst_out, dst_out, dstt_out):
    rows, width = src_out.shape
    wide = res_ref.shape[1]
    lane = lax.broadcasted_iota(jnp.int32, (rows, wide), 1)
    for first, out in ((0, src_out), (rows, dst_out)):
        x = res_ref[first:first + rows]
        im = pltpu.roll(x, wide // 2 + half, axis=1)
        out[...] = jnp.where(lane < half, x, im)[:, :width]
    sst_out[...] = res_ref[2 * rows:2 * rows + 1, 0:rows]
    dstt_out[...] = res_ref[2 * rows + 1:2 * rows + 2, 0:rows]


def solution(mesh):
    doms, edge_axis = mesh.shape["dom"], mesh.shape["edge"]
    chips = edge_axis // 2

    def on_device(
        src_table, src_state, dst_table, dst_state, relations, edge_src, edge_rel, edge_dst, negatives
    ):
        rows, width = src_table.shape
        half = width // 2
        wide = 2 * up(half, 128)
        ents = rows * edge_axis
        edges = edge_src.shape[1]
        ep = up(edges, 128)
        nrel = relations.shape[0]
        vm, dma = pltpu.VMEM, pltpu.SemaphoreType.DMA
        in_vmem = pl.BlockSpec(memory_space=pltpu.VMEM)
        in_hbm = pl.BlockSpec(memory_space=pltpu.HBM)
        shards = rows // 16
        block = (shards, MSG, 128)
        shard = jax.ShapeDtypeStruct((rows, width), F32)
        line = jax.ShapeDtypeStruct((1, rows), F32)
        packed = pl.pallas_call(
            functools.partial(kernel, doms, chips, half),
            out_shape=jax.ShapeDtypeStruct((2 * rows + 8, wide), F32),
            in_specs=[in_hbm] * 9,
            out_specs=in_vmem,
            scratch_shapes=[
                vm((rows, width), F32),
                vm((1, rows), F32),
                vm((rows, width), F32),
                vm((1, rows), F32),
                vm((2, edges), jnp.int32),
                pltpu.SMEM((2, edges), jnp.int32),
                vm((2, edges), jnp.int32),
                vm(negatives.shape, jnp.int32),
                vm((width, nrel), F32),
                vm((width, 128), F32),
                vm((up(nrel, 128), wide), F32),
                vm((2, ep, wide), F32),
                vm((2, ep, ents), BF),
                vm((2, ents, ep), BF),
                vm((2, ents, ep), F32),
                vm((2, ents, ep), F32),
                vm((3, 1, ep), jnp.int32),
            ]
            + [vm((2, rows, wide), F32)] * 2
            + [vm((2,) + block, F32)] * 2
            + [vm((2, edge_axis) + block, F32)] * 2
            + [vm((2, ents // 2, wide), F32)] * 4
            + [vm((2, chips) + block, F32)] * 4
            + [vm((ep, wide), BF)] * 2
            + [vm((ents, wide), BF)] * 4
            + [vm((ents, ep), BF)] * 2
            + [vm((ep, ents), BF)] * 2
            + [dma((8,))] * 2
            + [dma((2, chips))] * 8
            + [dma((2, 2))] * 2
            + [dma((2, chips))] * 4,
            compiler_params=pltpu.CompilerParams(
                collective_id=0, has_side_effects=True, vmem_limit_bytes=50 * 1024 * 1024
            ),
        )(
            *(pltpu.with_memory_space_constraint(a, pltpu.HBM) for a in (
            src_table,
            src_state.reshape(1, rows),
            dst_table,
            dst_state.reshape(1, rows),
            relations.T,
            edge_src,
            edge_rel,
            edge_dst,
            negatives,
            )),
        )
        out = pl.pallas_call(
            functools.partial(finish, half),
            out_shape=(shard, line, shard, line),
            in_specs=[in_vmem],
            out_specs=(in_vmem,) * 4,
            compiler_params=pltpu.CompilerParams(vmem_limit_bytes=1024 * 1024),
        )(packed)
        return out[0], out[1].reshape(rows), out[2], out[3].reshape(rows)

    return jax.shard_map(
        on_device,
        mesh=mesh,
        in_specs=(
            P(("dom", "edge"), None),
            P(("dom", "edge")),
            P(("dom", "edge"), None),
            P(("dom", "edge")),
            P(),
            P(None, ("dom", "edge")),
            P(None, ("dom", "edge")),
            P(None, ("dom", "edge")),
            P(None, ("dom", "edge"), None),
        ),
        out_specs=(
            P(("dom", "edge"), None),
            P(("dom", "edge")),
            P(("dom", "edge"), None),
            P(("dom", "edge")),
        ),
        check_vma=False,
    )
```

```python
import functools

import jax
import jax.numpy as jnp
from jax import lax
from jax.experimental import pallas as pl
from jax.experimental.pallas import tpu as pltpu
from jax.sharding import PartitionSpec as P

MESH = pl.DeviceIdType.MESH
LEARN_RATE = 0.1
EPSILON = 1e-06
MSG = 50
BF = jnp.bfloat16
F32 = jnp.float32


def up(n, m):
    return (n + m - 1) // m * m


def halves(x):
    hi = x.astype(BF)
    return hi, (x - hi.astype(F32)).astype(BF)


def nn(a, b):
    return jnp.dot(a, b, preferred_element_type=F32)


def nt(a, b):
    return lax.dot_general(a, b, (((1,), (1,)), ((), ())), preferred_element_type=F32)


def lanes(n):
    return lax.broadcasted_iota(jnp.int32, (n, 128), 1)


def packed_rows(x):
    a0, a1, b0, b1 = (x[:, n * 128:(n + 1) * 128] for n in range(4))
    lane = lanes(x.shape[0])
    both = jnp.where(lane < 64, a1, pltpu.roll(b1, 64, axis=1))
    left = jnp.where(lane < 8, pltpu.roll(a1, 64, axis=1), jnp.where(lane < 16, pltpu.roll(b1, 72, axis=1), 0.0))
    for n in (16, 32, 64):
        left = left + pltpu.roll(left, n, axis=1)
    line = lax.rem(lax.broadcasted_iota(jnp.int32, lane.shape, 0), 8)
    left = jnp.where(lax.div(lane, 16) == 7 - line, left, 0.0)
    tails = [jnp.sum(left[t:t + 8], axis=0, keepdims=True) for t in range(0, x.shape[0], 8)]
    return a0, b0, both, tails


def put_packed(ref, x):
    a0, b0, both, tails = packed_rows(x)
    n = x.shape[0]
    ref[0:n] = a0
    ref[n:2 * n] = b0
    ref[2 * n:3 * n] = both
    for t, row in enumerate(tails):
        ref[3 * n + t:3 * n + t + 1] = row


def unpacked(x, tails):
    n = x.shape[0] // 3
    lane = lanes(n)
    a0, b0, both = x[0:n], x[n:2 * n], x[2 * n:3 * n]
    re = []
    for row in tails:
        v = jnp.broadcast_to(pltpu.roll(row, 80, axis=1), (8, 128))
        re.append(pltpu.roll(v, 0, axis=1, stride=16, stride_axis=0))
    re = jnp.concatenate(re, axis=0)
    im = pltpu.roll(re, 120, axis=1)
    a1 = jnp.where(lane < 64, both, jnp.where(lane < 72, re, 0.0))
    b1 = jnp.where(lane < 64, pltpu.roll(both, 64, axis=1), jnp.where(lane < 72, im, 0.0))
    return jnp.concatenate([a0, a1, b0, b1], axis=1)


def tail_rows(x_ref, n):
    return [x_ref[3 * n + t:3 * n + t + 1] for t in range(n // 8)]


def kernel(
    doms, chips, half,
    src_hbm, sst_hbm, dst_hbm, dstt_hbm, rel_hbm, es_hbm, er_hbm, ed_hbm, ng_hbm,
    out_ref,
    src_ref, sst_ref, dst_ref, dstt_ref, es_ref, er_ref, ed_ref, ng_ref,
    rel_t, rel_e, rel_v, rsp, hot, hot_t, wgt, pos, ids,
    tab_s, tab_d, own_s, own_d, full_s, full_d, part_s, part_d, sib_s, sib_d, sum_s, sum_d, red_s, red_d,
    qh, ql, dh, dl, th, tl, wth, wtl, wh, wl,
    in_sem, rel_sem, ags_send, ags_recv, agd_send, agd_recv, fws_send, fws_recv, fwd_send, fwd_recv,
    dd_send, dd_recv, rss_send, rss_recv, rsd_send, rsd_recv,
):
    rows, width = src_ref.shape
    hp = up(half, 128)
    wide = 2 * hp
    ents = th.shape[0]
    hent = ents // 2
    shards = rows // 16
    edges = es_ref.shape[1]
    ep = rsp.shape[1]
    nrel = rel_hbm.shape[1]
    shift = hp - half

    dom = lax.axis_index("dom")
    k = lax.axis_index("edge")
    core = lax.rem(k, 2)
    chip = lax.div(k, 2)
    mate = chip * 2 + (1 - core)
    nx = chips // 2

    def at_dom(step):
        return lax.rem(dom + step + doms, doms)

    def far(o):
        return min(o[0], nx - o[0]) + 2 * o[1]

    offsets = sorted(((dx, dy) for dx in range(nx) for dy in range(2)), key=lambda o: -far(o))
    others = [o for o in offsets if o != (0, 0)]

    def peer(o):
        return lax.rem(lax.div(chip, 2) + o[0], nx) * 2 + lax.rem(lax.rem(chip, 2) + o[1], 2)

    bar = pltpu.get_barrier_semaphore()
    count = 1
    for other in (at_dom(1), at_dom(-1)):
        for o in offsets:
            pl.semaphore_signal(bar, inc=1, device_id=(other, peer(o) * 2 + core), device_id_type=MESH)
            count += 1
    for o in others:
        pl.semaphore_signal(bar, inc=1, device_id=(dom, peer(o) * 2 + core), device_id_type=MESH)
        count += 1
    pl.semaphore_signal(bar, inc=1, device_id=(dom, mate), device_id_type=MESH)

    inputs = []
    for n, (a, b) in enumerate((
        (src_hbm, src_ref), (dst_hbm, dst_ref), (sst_hbm, sst_ref), (dstt_hbm, dstt_ref),
        (es_hbm, es_ref), (er_hbm, er_ref), (ed_hbm, ed_ref), (ng_hbm, ng_ref),
    )):
        c = pltpu.make_async_copy(a, b, in_sem.at[n])
        c.start()
        inputs.append(c)
    piece = up(-(-width // rel_sem.shape[0]), 8)
    rel_copies = []
    for n in range(rel_sem.shape[0]):
        lo = n * piece
        size = min(piece, width - lo)
        if size > 0:
            c = pltpu.make_async_copy(
                rel_hbm.at[pl.ds(lo, size)], rel_t.at[pl.ds(lo, size)], rel_sem.at[n])
            c.start()
            rel_copies.append(c)

    lane = lax.broadcasted_iota(jnp.int32, (rows, wide), 1)

    def put_table(step, table, tab, own):
        tab[step] = table
        for n in range(shards):
            put_packed(own.at[step, n], table[n * 16:n * 16 + 16])

    def spread(x_ref, tab, own):
        tab[0] = jnp.zeros((rows, wide), F32)
        tab[0, :, 0:width] = x_ref[...]
        x = tab[0]
        im = pltpu.roll(x, shift, axis=1)
        put_table(0, jnp.where(lane < half, x, jnp.where(lane >= hp, im, 0.0)), tab, own)

    for c in inputs[:2]:
        c.wait()
    spread(src_ref, tab_s, own_s)
    spread(dst_ref, tab_d, own_d)

    eye = lax.broadcasted_iota(jnp.int32, (rows, rows), 0) == lax.broadcasted_iota(jnp.int32, (rows, rows), 1)

    def column(x_ref):
        return jnp.sum(jnp.where(eye, jnp.broadcast_to(x_ref[...], (rows, rows)), 0.0), axis=1, keepdims=True)

    def as_row(x):
        return jnp.sum(jnp.where(eye, jnp.broadcast_to(x, (rows, rows)), 0.0), axis=0, keepdims=True)

    mine = core * chips + chip

    def gather_src(step):
        out = []
        for n, o in enumerate(others):
            c = pltpu.make_async_remote_copy(
                own_s.at[step], full_s.at[step, mine], ags_send.at[step, n], ags_recv.at[step, chip],
                device_id=(dom, peer(o) * 2 + core), device_id_type=MESH)
            c.start()
            out.append(c)
        c = pltpu.make_async_remote_copy(
            own_s.at[step], full_s.at[step, mine], fws_send.at[step, chip], fws_recv.at[step, chip],
            device_id=(dom, mate), device_id_type=MESH)
        c.start()
        out.append(c)
        full_s[step, mine] = own_s[step]
        return out

    def gather_dst(step):
        out = []
        for n, o in enumerate(offsets):
            c = pltpu.make_async_remote_copy(
                own_d.at[step], full_d.at[step, mine], agd_send.at[step, n], agd_recv.at[step, chip],
                device_id=(at_dom(step + 1), peer(o) * 2 + core), device_id_type=MESH)
            c.start()
            out.append(c)
        return out

    def forward(step, full, recv, fsend, frecv, which):
        out = []
        for o in reversed(which):
            c = peer(o)
            blk = full.at[step, core * chips + c]
            pltpu.make_async_copy(blk, blk, recv.at[step, c]).wait()
            f = pltpu.make_async_remote_copy(
                blk, blk, fsend.at[step, c], frecv.at[step, c], device_id=(dom, mate), device_id_type=MESH)
            f.start()
            out.append(f)
        return out

    def from_mate(step, full, frecv):
        for c in range(chips):
            blk = full.at[step, (1 - core) * chips + c]
            pltpu.make_async_copy(blk, blk, frecv.at[step, c]).wait()

    def place(x):
        per = rows * 2
        return lax.rem(lax.div(x, rows), 2) * hent + lax.div(x, per) * rows + lax.rem(x, rows)

    def turn_relations():
        fill = jnp.zeros((hp - half, 128), F32)
        full = nrel // 128

        def turned(ref, cols, to):
            rel_v[to, 0:hp] = jnp.concatenate([ref[0:half, cols], fill], axis=0).T
            rel_v[to, hp:wide] = jnp.concatenate([ref[half:width, cols], fill], axis=0).T

        def body(b, carry):
            cols = pl.ds(pl.multiple_of(b * 128, 128), 128)
            turned(rel_t, cols, cols)
            return carry

        lax.fori_loop(0, full, body, 0)
        if nrel % 128:
            rel_e[...] = jnp.zeros((width, 128), F32)
            rel_e[:, 0:nrel % 128] = rel_t[:, full * 128:nrel]
            turned(rel_e, slice(0, 128), slice(full * 128, full * 128 + 128))

    def prepare(step):
        tail = edges // 8 * 8
        rsp[step, tail:ep] = jnp.zeros((ep - tail, wide), F32)
        unroll = 20

        def body(b, carry):
            for u in range(unroll):
                e = b * unroll + u
                i = er_ref[step, e]
                rsp[step, pl.ds(e, 1), :] = rel_v[pl.ds(i, 1), :]
            return carry

        lax.fori_loop(0, edges // unroll, body, 0)

        def hots(ref, slot):
            ids[slot] = jnp.full((1, ep), -1, jnp.int32)
            ids[slot, :, 0:edges] = ref[step] if len(ref.shape) == 3 else ref[step:step + 1, :]
            x = ids[slot]
            return jnp.where(x < 0, -1, place(jnp.maximum(x, 0)))

        xs, xd, xn = hots(es_ref, 0), hots(ed_ref, 1), hots(ng_ref, 2)
        for m in range(0, ents, 128):
            line = lax.broadcasted_iota(jnp.int32, (128, ep), 0) + m
            s = jnp.where(line == xs, 1.0, 0.0)
            hot_t[step, m:m + 128] = s.astype(BF)
            hot[step, :, m:m + 128] = s.T.astype(BF)
            d = jnp.where(line == xd, 1.0, 0.0)
            c = jnp.sum(jnp.where(line == xn, 1.0, 0.0), axis=1, keepdims=True)
            pos[step, m:m + 128] = d
            wgt[step, m:m + 128] = d + c

    lower = pl.ds(pl.multiple_of(core * hent, hent), hent)
    upper = pl.ds(pl.multiple_of((1 - core) * hent, hent), hent)

    def split_to(full, step, side, a, b):
        for c in range(chips):
            for n in range(shards):
                blk = full.at[step, side * chips + c, n]
                at = pl.ds(pl.multiple_of(side * hent + c * rows + n * 16, 16), 16)
                a[at], b[at] = halves(unpacked(blk[0:48], tail_rows(blk, 16)))

    def rotated(step):
        for m in range(0, ep, 128):
            o = hot[step, m:m + 128]
            s = nn(o, th[...]) + nn(o, tl[...])
            sr, si = s[:, :hp], s[:, hp:]
            rr, ri = rsp[step, m:m + 128, :hp], rsp[step, m:m + 128, hp:]
            qh[m:m + 128, :hp], ql[m:m + 128, :hp] = halves(sr * rr - si * ri)
            qh[m:m + 128, hp:], ql[m:m + 128, hp:] = halves(sr * ri + si * rr)

    def weights(step, side):
        for m in range(0, hent, 128):
            at = pl.ds(pl.multiple_of(side * hent + m, 128), 128)
            a, b = dh[at], dl[at]
            s = nt(a, qh[...]) + (nt(a, ql[...]) + nt(b, qh[...]))
            w = (0.5 * jnp.tanh(0.5 * s) + 0.5) * wgt[step, at] - pos[step, at]
            wth[at], wtl[at] = halves(w)

    def dst_part(which):
        a, b = wth[which], wtl[which]
        return nn(a, qh[...]) + (nn(a, ql[...]) + nn(b, qh[...]))

    def edge_grads(step):
        for m in range(0, ents, 128):
            wh[:, m:m + 128] = wth[m:m + 128].T
            wl[:, m:m + 128] = wtl[m:m + 128].T
        for m in range(0, ep, 128):
            a, b = wh[m:m + 128], wl[m:m + 128]
            g = nn(a, dh[...]) + (nn(a, dl[...]) + nn(b, dh[...]))
            gr, gi = g[:, :hp], g[:, hp:]
            rr, ri = rsp[step, m:m + 128, :hp], rsp[step, m:m + 128, hp:]
            qh[m:m + 128, :hp], ql[m:m + 128, :hp] = halves(gr * rr + gi * ri)
            qh[m:m + 128, hp:], ql[m:m + 128, hp:] = halves(gi * rr - gr * ri)

    def src_part(step, which):
        o = hot_t[step, which]
        return nn(o, qh[...]) + nn(o, ql[...])

    def to_mate(step, t, part, sib):
        c = pltpu.make_async_remote_copy(
            part.at[step], sib.at[step], dd_send.at[step, t], dd_recv.at[step, t],
            device_id=(dom, mate), device_id_type=MESH)
        c.start()
        return c

    def to_owners(step, copy, part, sib, total, red, send, recv, target, which):
        copy.wait_recv()
        for c in range(chips):
            for n in range(shards):
                at = slice(c * rows + n * 16, c * rows + n * 16 + 16)
                put_packed(total.at[step, c, n], part[at] + sib[step, at])
        out = []
        for n, o in enumerate(which):
            c = peer(o)
            r = pltpu.make_async_remote_copy(
                total.at[step, c], red.at[step, chip], send.at[step, n], recv.at[step, chip],
                device_id=(target, c * 2 + core), device_id_type=MESH)
            r.start()
            out.append(r)
        if len(which) < chips:
            red[step, chip] = total[step, chip]
        return out

    def arrived(step, red, recv, which):
        for o in reversed(which):
            blk = red.at[step, peer(o)]
            pltpu.make_async_copy(blk, blk, recv.at[step, peer(o)]).wait()
        out = []
        for n in range(shards):
            g, tails = red[step, 0, n, 0:48], tail_rows(red.at[step, 0, n], 16)
            for c in range(1, chips):
                g = g + red[step, c, n, 0:48]
                tails = [t + u for t, u in zip(tails, tail_rows(red.at[step, c, n], 16))]
            out.append(unpacked(g, tails))
        return out[0] if shards == 1 else jnp.concatenate(out, axis=0)

    def adagrad(table, state, g):
        state = state + jnp.sum(g * g, axis=1, keepdims=True) / width
        return table - LEARN_RATE * g / (jnp.sqrt(state) + EPSILON), state

    pl.semaphore_wait(bar, count)

    sent = []
    sent += gather_dst(0)
    sent += gather_src(0)
    for c in inputs[2:] + rel_copies:
        c.wait()
    src_state = column(sst_ref)
    dst_state = column(dstt_ref)
    turn_relations()
    prepare(0)

    for step in range(2):
        if step == 0:
            sent += forward(step, full_s, ags_recv, fws_send, fws_recv, others)
            sent += forward(step, full_d, agd_recv, fwd_send, fwd_recv, offsets)
            split_to(full_s, step, core, th, tl)
            split_to(full_d, step, core, dh, dl)
            from_mate(step, full_s, fws_recv)
            split_to(full_s, step, 1 - core, th, tl)
            rotated(step)
            weights(step, core)
            from_mate(step, full_d, fwd_recv)
            split_to(full_d, step, 1 - core, dh, dl)
        else:
            sent += forward(step, full_d, agd_recv, fwd_send, fwd_recv, offsets)
            sent += forward(step, full_s, ags_recv, fws_send, fws_recv, others)
            split_to(full_s, step, core, th, tl)
            split_to(full_d, step, core, dh, dl)
            from_mate(step, full_d, fwd_recv)
            split_to(full_d, step, 1 - core, dh, dl)
            from_mate(step, full_s, fws_recv)
            split_to(full_s, step, 1 - core, th, tl)
            rotated(step)
        weights(step, 1 - core)
        part_d[step] = dst_part(upper)
        cd = to_mate(step, 0, part_d, sib_d)
        if step == 1:
            weights(step, core)
        mine_d = dst_part(lower)
        edge_grads(step)
        part_s[step] = src_part(step, upper)
        cs = to_mate(step, 1, part_s, sib_s)
        sent += to_owners(step, cd, mine_d, sib_d, sum_d, red_d, rsd_send, rsd_recv, at_dom(-step - 1), offsets)
        mine_s = src_part(step, lower)
        sent += to_owners(step, cs, mine_s, sib_s, sum_s, red_s, rss_send, rss_recv, dom, others)
        if step == 0:
            prepare(1)
        g = arrived(step, red_d, rsd_recv, offsets)
        table, dst_state = adagrad(tab_d[step], dst_state, g)
        if step == 0:
            put_table(1, table, tab_d, own_d)
            sent += gather_dst(1)
        else:
            out_ref[rows:2 * rows] = table
            out_ref[2 * rows + 1:2 * rows + 2, 0:rows] = as_row(dst_state)
        g = arrived(step, red_s, rss_recv, others)
        table, src_state = adagrad(tab_s[step], src_state, g)
        if step == 0:
            put_table(1, table, tab_s, own_s)
            sent += gather_src(1)
        else:
            out_ref[0:rows] = table
            out_ref[2 * rows:2 * rows + 1, 0:rows] = as_row(src_state)
        sent += [cd, cs]
    for c in sent:
        c.wait_send()


def finish(half, res_ref, src_out, sst_out, dst_out, dstt_out):
    rows, width = src_out.shape
    wide = res_ref.shape[1]
    lane = lax.broadcasted_iota(jnp.int32, (rows, wide), 1)
    for first, out in ((0, src_out), (rows, dst_out)):
        x = res_ref[first:first + rows]
        im = pltpu.roll(x, wide // 2 + half, axis=1)
        out[...] = jnp.where(lane < half, x, im)[:, :width]
    sst_out[...] = res_ref[2 * rows:2 * rows + 1, 0:rows]
    dstt_out[...] = res_ref[2 * rows + 1:2 * rows + 2, 0:rows]


def solution(mesh):
    doms, edge_axis = mesh.shape["dom"], mesh.shape["edge"]
    chips = edge_axis // 2

    def on_device(
        src_table, src_state, dst_table, dst_state, relations, edge_src, edge_rel, edge_dst, negatives
    ):
        rows, width = src_table.shape
        half = width // 2
        wide = 2 * up(half, 128)
        ents = rows * edge_axis
        edges = edge_src.shape[1]
        ep = up(edges, 128)
        nrel = relations.shape[0]
        vm, dma = pltpu.VMEM, pltpu.SemaphoreType.DMA
        in_vmem = pl.BlockSpec(memory_space=pltpu.VMEM)
        in_hbm = pl.BlockSpec(memory_space=pltpu.HBM)
        shards = rows // 16
        block = (shards, MSG, 128)
        shard = jax.ShapeDtypeStruct((rows, width), F32)
        line = jax.ShapeDtypeStruct((1, rows), F32)
        packed = pl.pallas_call(
            functools.partial(kernel, doms, chips, half),
            out_shape=jax.ShapeDtypeStruct((2 * rows + 8, wide), F32),
            in_specs=[in_hbm] * 9,
            out_specs=in_vmem,
            scratch_shapes=[
                vm((rows, width), F32),
                vm((1, rows), F32),
                vm((rows, width), F32),
                vm((1, rows), F32),
                vm((2, edges), jnp.int32),
                pltpu.SMEM((2, edges), jnp.int32),
                vm((2, edges), jnp.int32),
                vm(negatives.shape, jnp.int32),
                vm((width, nrel), F32),
                vm((width, 128), F32),
                vm((up(nrel, 128), wide), F32),
                vm((2, ep, wide), F32),
                vm((2, ep, ents), BF),
                vm((2, ents, ep), BF),
                vm((2, ents, ep), F32),
                vm((2, ents, ep), F32),
                vm((3, 1, ep), jnp.int32),
            ]
            + [vm((2, rows, wide), F32)] * 2
            + [vm((2,) + block, F32)] * 2
            + [vm((2, edge_axis) + block, F32)] * 2
            + [vm((2, ents // 2, wide), F32)] * 4
            + [vm((2, chips) + block, F32)] * 4
            + [vm((ep, wide), BF)] * 2
            + [vm((ents, wide), BF)] * 4
            + [vm((ents, ep), BF)] * 2
            + [vm((ep, ents), BF)] * 2
            + [dma((8,))] * 2
            + [dma((2, chips))] * 8
            + [dma((2, 2))] * 2
            + [dma((2, chips))] * 4,
            compiler_params=pltpu.CompilerParams(
                collective_id=0, has_side_effects=True, vmem_limit_bytes=50 * 1024 * 1024
            ),
        )(
            *(pltpu.with_memory_space_constraint(a, pltpu.HBM) for a in (
            src_table,
            src_state.reshape(1, rows),
            dst_table,
            dst_state.reshape(1, rows),
            relations.T,
            edge_src,
            edge_rel,
            edge_dst,
            negatives,
            )),
        )
        out = pl.pallas_call(
            functools.partial(finish, half),
            out_shape=(shard, line, shard, line),
            in_specs=[in_vmem],
            out_specs=(in_vmem,) * 4,
            compiler_params=pltpu.CompilerParams(vmem_limit_bytes=1024 * 1024),
        )(packed)
        return out[0], out[1].reshape(rows), out[2], out[3].reshape(rows)

    return jax.shard_map(
        on_device,
        mesh=mesh,
        in_specs=(
            P(("dom", "edge"), None),
            P(("dom", "edge")),
            P(("dom", "edge"), None),
            P(("dom", "edge")),
            P(),
            P(None, ("dom", "edge")),
            P(None, ("dom", "edge")),
            P(None, ("dom", "edge")),
            P(None, ("dom", "edge"), None),
        ),
        out_specs=(
            P(("dom", "edge"), None),
            P(("dom", "edge")),
            P(("dom", "edge"), None),
            P(("dom", "edge")),
        ),
        check_vma=False,
    )
```
